256 devices in a mesh: section: 32 (over x, z_hi, core), dp: 8 (over z_lo, y).
Axes of the slice: x: 4, y: 4, z: 8 (z_hi: 4, z_lo: 2; z = z_hi * 2 + z_lo), core: 2. Of those that a mesh axis runs over, the one named last changes fastest.
Arguments:
- w_value: bfloat16 [32, 2, 4608, 1024], P('section', None, None, 'dp'), may hold values from -0.09375 to 0.09375
- w_out: bfloat16 [32, 2, 1024, 4608], P('section', None, 'dp'), may hold values from -0.1875 to 0.1875
- norm_gain: float32 [32, 2, 4608], P('section'), may hold values from 0.5 to 1.5
- saved_inputs: bfloat16 [32, 3, 2, 64, 4608], P('section', None, None, 'dp'), may hold values from -6 to 6
- arriving: bfloat16 [32, 2, 64, 4608], P('section', None, 'dp'), may hold values from -6 to 6
- returning: bfloat16 [32, 2, 64, 4608], P('section', None, 'dp'), may hold values from -6 to 6
- fresh_rows: bfloat16 [4, 64, 4608], P(None, 'dp'), may hold values from -6 to 6
- targets: bfloat16 [4, 64, 4608], P(None, 'dp'), may hold values from -6 to 6
- fill_slots: int32 [32, 4, 2], P('section'), may hold values from 0 to 2
- read_slots: int32 [32, 4, 2], P('section'), may hold values from 0 to 2
Outputs:
- activ_out: bfloat16 [32, 2, 64, 4608], P('section', None, 'dp')
- cotan_out: bfloat16 [32, 2, 64, 4608], P('section', None, 'dp')
- stash_out: bfloat16 [32, 3, 2, 64, 4608], P('section', None, None, 'dp')
- grad_value: bfloat16 [32, 2, 4608, 1024], P('section', None, None, 'dp')
- grad_out: bfloat16 [32, 2, 1024, 4608], P('section', None, 'dp')
- grad_gain: float32 [32, 2, 4608], P('section')
The draws below stay inside these ranges and needn't reach their ends.
All inputs are finite; a program needn't handle non-finite values.
Results may differ from the reference program's by a relative error of at most 0.029.
Values may be sent and summed in bfloat16 or wider, within the bound.
A program may use at most 128 MiB of HBM per device.

```python
import jax
import jax.numpy as jnp
from jax import lax

D = 4608
K = 1024
TICKS = 4
SLOTS = 3
ROWS = 64
N_SECTION = 32
N_DP = 8


def set_ends(drawn, stream_key, smallest, top_value):
    extent = drawn.shape
    place = [jax.random.randint(jax.random.fold_in(stream_key, axis), (), 0, extent[axis]) for axis in range(len(extent))]
    drawn = drawn.at[tuple(place)].set(smallest)
    longest = extent.index(max(extent))
    place[longest] = (place[longest] + 1) % extent[longest]
    return drawn.at[tuple(place)].set(top_value)


def block_scale(rng, dims, cuts, low, high):
    gain, own = 1.0, jax.random.fold_in(rng, 6)
    for position, shards_of in cuts:
        steps = jnp.exp(jax.random.uniform(jax.random.fold_in(own, position), (shards_of,), jnp.float32, low / len(cuts), high / len(cuts)))
        gain = gain * jnp.repeat(steps, dims[position] // shards_of).reshape([-1 if axis == position else 1 for axis in range(len(dims))])
    return gain


def scatter_about(key, shape, deviation, reach, cuts=(), held_as=jnp.bfloat16):
    values = jax.random.normal(key, shape, jnp.float32) * deviation
    if len(cuts) > 0:
        values = block_scale(key, shape, cuts, -0.22, 0.18) * values
    return jnp.clip(values, min=-reach, max=reach).astype(held_as)


def setup_inputs(seed: int = 0) -> dict:
    key_of = jax.random.split(jax.random.key(seed), 11)
    w_value = scatter_about(key_of[0], (N_SECTION, 2, D, K), D ** -0.5, 0.09375, ((0, 32), (3, 8)))
    w_out = scatter_about(key_of[1], (N_SECTION, 2, K, D), K ** -0.5, 0.1875, ((0, 32), (2, 8)))
    norm_gain = jnp.clip(1.0 + 0.1 * jax.random.normal(key_of[2], (N_SECTION, 2, D), jnp.float32), 0.5, 1.5)
    saved_inputs = scatter_about(key_of[3], (N_SECTION, SLOTS, 2, ROWS, D), 1.0, 6.0, ((0, 32), (3, 8)))
    arriving = scatter_about(key_of[4], (N_SECTION, 2, ROWS, D), 1.0, 6.0, ((0, 32), (2, 8)))
    returning = scatter_about(key_of[5], (N_SECTION, 2, ROWS, D), 1.0, 6.0, ((0, 32), (2, 8)))
    fresh_rows = scatter_about(key_of[6], (TICKS, ROWS, D), 1.0, 6.0, ((1, 8),))
    targets = scatter_about(key_of[7], (TICKS, ROWS, D), 1.0, 6.0, ((1, 8),))
    fill_slots = set_ends(jax.random.randint(key_of[8], (N_SECTION, TICKS, 2), 0, SLOTS), jax.random.fold_in(key_of[8], 1), 0, SLOTS - 1).astype(jnp.int32)
    read_slots = set_ends(jax.random.randint(key_of[9], (N_SECTION, TICKS, 2), 0, SLOTS), jax.random.fold_in(key_of[9], 1), 0, SLOTS - 1).astype(jnp.int32)
    return dict(w_value=w_value, w_out=w_out, norm_gain=norm_gain, saved_inputs=saved_inputs, arriving=arriving, returning=returning, fresh_rows=fresh_rows, targets=targets, fill_slots=fill_slots, read_slots=read_slots)


epsilon = 1e-06

def exact_dot(left, right):
    return jnp.dot(left.astype(jnp.float32), right.astype(jnp.float32), precision=lax.Precision.HIGHEST)

def normalize(block_rows, gain_row):
    values = block_rows.astype(jnp.float32)
    inv_root = lax.rsqrt(lax.optimization_barrier(jnp.mean(values * values, axis=-1, keepdims=True)) + epsilon)
    scaled = values * inv_root
    return (scaled, inv_root, (scaled * gain_row).astype(jnp.bfloat16))

def shard_sums(left, right):
    pieces = right.shape[0] // N_DP
    split_left = left.astype(jnp.float32).reshape(left.shape[0], N_DP, pieces)
    split_right = right.astype(jnp.float32).reshape(N_DP, pieces, right.shape[1])
    terms = jnp.einsum('rjk,jkd->jrd', split_left, split_right, precision=lax.Precision.HIGHEST)
    rounded = lax.optimization_barrier(terms.astype(jnp.bfloat16))
    return lax.optimization_barrier(jnp.sum(rounded.astype(jnp.float32), axis=0))

def forward_layer(block_rows, gain_row, value_mat, out_mat):
    scaled, inv_root, normed = normalize(block_rows, gain_row)
    values = exact_dot(normed, value_mat).astype(jnp.bfloat16)
    return (block_rows.astype(jnp.float32) + shard_sums(values, out_mat)).astype(jnp.bfloat16)

def backward_layer(source, upstream, gain_row, value_mat, out_mat):
    scaled, inv_root, normed = normalize(source, gain_row)
    down_grad = exact_dot(upstream, out_mat.T).astype(jnp.bfloat16)
    pulled = shard_sums(down_grad, value_mat.T)
    weighted = pulled * gain_row
    inner_mean = lax.optimization_barrier(jnp.mean(weighted * scaled, axis=-1, keepdims=True))
    grad_in = (upstream.astype(jnp.float32) + inv_root * (weighted - scaled * inner_mean)).astype(jnp.bfloat16)
    values = exact_dot(normed, value_mat).astype(jnp.bfloat16)
    return (grad_in, exact_dot(normed.T, down_grad), exact_dot(values.T, upstream), lax.optimization_barrier(jnp.sum(pulled * scaled, axis=0)))

def section_work(entries):
    inputs_now, upstream_now, sources, gains, value_mats, out_mats = entries
    layer_outs, grad_ins, value_terms, out_terms, gain_terms = ([], [], [], [], [])
    for group in range(2):
        layer_outs.append(forward_layer(inputs_now[group], gains[group], value_mats[group], out_mats[group]))
        grad_in, value_term, out_term, gain_term = backward_layer(sources[group], upstream_now[group], gains[group], value_mats[group], out_mats[group])
        grad_ins.append(grad_in)
        value_terms.append(value_term)
        out_terms.append(out_term)
        gain_terms.append(gain_term)
    return (jnp.stack(layer_outs), jnp.stack(grad_ins), jnp.stack(value_terms), jnp.stack(out_terms), jnp.stack(gain_terms))

def reference(w_value, w_out, norm_gain, saved_inputs, arriving, returning, fresh_rows, targets, fill_slots, read_slots):
    activations = arriving
    cotangents = returning
    saved = saved_inputs
    value_sums = jnp.zeros(w_value.shape, jnp.float32)
    out_sums = jnp.zeros(w_out.shape, jnp.float32)
    gain_sums = jnp.zeros(norm_gain.shape, jnp.float32)
    slot_ids = jnp.arange(SLOTS, dtype=jnp.int32)
    outputs = activations
    gradients = cotangents
    for tick_index in range(TICKS):
        if tick_index > 0:
            lower_group = jnp.concatenate([fresh_rows[tick_index][None], outputs[:-1, 0]], axis=0)
            upper_group = jnp.concatenate([outputs[-1:, 0], outputs[:-1, 1]], axis=0)
            activations = jnp.stack([lower_group, upper_group], axis=1)
            finish = (outputs[-1, 1].astype(jnp.float32) - targets[tick_index - 1].astype(jnp.float32)).astype(jnp.bfloat16)
            lower_grad = jnp.concatenate([gradients[1:, 0], gradients[:1, 1]], axis=0)
            upper_grad = jnp.concatenate([gradients[1:, 1], finish[None]], axis=0)
            cotangents = jnp.stack([lower_grad, upper_grad], axis=1)
        written = slot_ids[None, :, None] == fill_slots[:, tick_index, :][:, None, :]
        saved = jnp.where(written[:, :, :, None, None], activations[:, None], saved)
        chosen = slot_ids[None, :, None] == read_slots[:, tick_index, :][:, None, :]
        sources = lax.optimization_barrier(jnp.sum(jnp.where(chosen[:, :, :, None, None], saved.astype(jnp.float32), jnp.zeros((), jnp.float32)), axis=1)).astype(jnp.bfloat16)
        outputs, gradients, value_terms, out_terms, gain_terms = lax.map(section_work, (activations, cotangents, sources, norm_gain, w_value, w_out))
        value_sums = value_sums + value_terms
        out_sums = out_sums + out_terms
        gain_sums = gain_sums + gain_terms
    grad_scale = (TICKS * ROWS) ** (-0.5)
    return (outputs, gradients, saved, (value_sums * grad_scale).astype(jnp.bfloat16), (out_sums * grad_scale).astype(jnp.bfloat16), gain_sums * grad_scale)
```

```python
import functools

import jax
import jax.numpy as jnp
from jax import lax
from jax.experimental import pallas as pl
from jax.experimental.pallas import tpu as pltpu
from jax.sharding import PartitionSpec as P

epsilon = 1e-06
MESH = pl.DeviceIdType.MESH
F32, BF16 = jnp.float32, jnp.bfloat16

F0, F1, B0, B1 = range(4)
YN, ZN = 4, 2


def dot_nn(a, b):
    return jnp.dot(a, b, preferred_element_type=F32)


def dot_nt(a, b):
    return lax.dot_general(a, b, (((1,), (1,)), ((), ())), preferred_element_type=F32)


def dot_tn(a, b):
    return lax.dot_general(a, b, (((0,), (0,)), ((), ())), preferred_element_type=F32)


def window(
    n_section,
    wv, wo, gain, saved, arr, ret, fresh, tgt, fill, read,
    act, cot, stash, gv, go, gg,
    nrm, cotf, nsv, xin, part, rsy, keep, zs, zr, ysnd, dsnd, shf, shb, dgs, gacc, gsum,
    ag_s, ag_r, rs_s, rs_r, sh_s, sh_r,
):
    ticks = fresh.shape[0]
    slots = saved.shape[0]
    depth = gain.shape[1]
    rows = arr.shape[1]
    tokens = rows * YN * ZN
    me = lax.axis_index("dp")
    sec = lax.axis_index("section")
    z, y = me // YN, me % YN
    zp = 1 - z
    first = sec == 0
    last = sec == n_section - 1
    nxt = lax.rem(sec + 1, n_section)
    prv = lax.rem(sec + n_section - 1, n_section)
    z_peer = {"dp": zp * YN + y}

    def y_at(k):
        return lax.rem(y + k, YN)

    def y_peer(k):
        return {"dp": z * YN + y_at(k)}

    barrier = pltpu.get_barrier_semaphore()
    for target in (y_peer(1), y_peer(2), y_peer(3), z_peer, {"section": nxt}, {"section": prv}):
        pl.semaphore_signal(barrier, inc=1, device_id=target, device_id_type=MESH)

    def send(src, dst, s, r, target):
        return pltpu.make_async_remote_copy(
            src_ref=src, dst_ref=dst, send_sem=s, recv_sem=r, device_id=target, device_id_type=MESH
        )

    def ag_own(buf, row, k):
        return send(buf.at[me], buf.at[me], ag_s.at[row, k], ag_r.at[row, me], y_peer(k) if k else z_peer)

    def ag_pass(buf, row, k):
        o = z * YN + y_at(k)
        return send(buf.at[o], buf.at[o], ag_s.at[row, YN - 1 + k], ag_r.at[row, o], z_peer)

    def ag_start(buf, row):
        for k in (2, 1, 3, 0):
            ag_own(buf, row, k).start()

    def ag_relay(buf, row):
        for k in (1, 3, 2):
            copy = ag_pass(buf, row, k)
            copy.wait_recv()
            copy.start()

    def ag_finish(buf, row):
        for k in (0, 1, 3, 2):
            o = zp * YN + y_at(k)
            send(buf.at[o], buf.at[o], ag_s.at[row, 0], ag_r.at[row, o], z_peer).wait_recv()

    def ag_drain(buf, row):
        for k in range(YN):
            ag_own(buf, row, k).wait_send()
        for k in range(1, YN):
            ag_pass(buf, row, k).wait_send()

    def rs_y(st, k):
        return send(part.at[st, :, y_at(k)], rsy.at[st, y], rs_s.at[st, k], rs_r.at[st, y], y_peer(k))

    def rs_z(st):
        return send(zs.at[st], zr.at[st], rs_s.at[st, 0], rs_r.at[st, YN], z_peer)

    def shift(st, t):
        g = st % 2
        if st < B0:
            return send(ysnd.at[t, g], shf.at[t, g], sh_s.at[t, st], sh_r.at[t, st], {"section": nxt})
        return send(dsnd.at[t, g], shb.at[t, g], sh_s.at[t, st], sh_r.at[t, st], {"section": prv})

    def normed_of(x, g):
        inv = lax.rsqrt(jnp.mean(x * x, axis=-1, keepdims=True) + epsilon)
        scaled = x * inv
        return scaled, inv, (scaled * gain[g : g + 1, :]).astype(BF16)

    def whole(ref, i):
        return ref[i].astype(F32).reshape(tokens, depth).astype(BF16)

    def buf_of(st, t):
        g = st % 2
        return (nrm if st < B0 else cotf).at[2 * t + g]

    def stage_s(st, t):
        g = st % 2
        if t > 0:
            shift(st, t - 1).wait_recv()
        if st < B0:
            if t == 0:
                x = arr[g].astype(F32)
            else:
                edge = fresh[t] if g == 0 else shf[t - 1, 0]
                x = jnp.where(first, edge.astype(F32), shf[t - 1, g].astype(F32))
            xin[t, g] = x.astype(BF16)
            own = normed_of(x, g)[2]
        elif t == 0:
            own = ret[g]
        else:
            if g == 0:
                edge = shb[t - 1, 1].astype(F32)
            else:
                edge = ysnd[t - 1, 1].astype(F32) - tgt[t - 1].astype(F32)
            own = jnp.where(last, edge, shb[t - 1, g].astype(F32)).astype(BF16)
        if t > 0:
            ag_drain(buf_of(st, t - 1), st)
        buf = buf_of(st, t)
        buf[me] = own
        ag_start(buf, st)

    def stage_relay(st, t):
        ag_relay(buf_of(st, t), st)

    def stage_c(st, t):
        g = st % 2
        ag_finish(buf_of(st, t), st)
        if st < B0:
            values = dot_nn(whole(nrm, 2 * t + g), wv[g]).astype(BF16)
            terms = dot_nn(values, wo[g])
        else:
            down = dot_nt(whole(cotf, 2 * t + g), wo[g]).astype(BF16)
            dgs[g, t * tokens : (t + 1) * tokens, :] = down
            terms = dot_nt(down, wv[g])
        if t > 0:
            for k in range(1, YN):
                rs_y(st, k).wait_send()
        part[st] = terms.reshape(ZN, YN, rows, depth).astype(BF16)
        for k in (2, 1, 3):
            rs_y(st, k).start()

    def stage_y(st, t):
        for k in (1, 3, 2):
            q = y_at(k)
            send(part.at[st, :, q], rsy.at[st, q], rs_s.at[st, k], rs_r.at[st, q], y_peer(k)).wait_recv()

        def total(zz):
            acc = part[st, zz, y].astype(F32)
            for k in range(1, YN):
                acc = acc + rsy[st, y_at(k), zz].astype(F32)
            return acc

        if t > 0:
            rs_z(st).wait_send()
        zs[st] = total(zp).astype(BF16)
        rs_z(st).start()
        keep[st] = total(z)

    def pick(candidates, which):
        chosen = candidates[0][1]
        for index, value in candidates[1:]:
            chosen = jnp.where(index == which, value, chosen)
        return chosen

    def source_rows(t, g):
        options = [(sl, saved[sl, g].astype(F32)) for sl in range(slots)]
        options += [(fill[u, g], xin[u, g].astype(F32)) for u in range(t + 1)]
        return pick(options, read[t, g])

    def stage_e(st, t):
        g = st % 2
        rs_z(st).wait_recv()
        total = keep[st] + zr[st].astype(F32)
        if st < B0:
            out = (xin[t, g].astype(F32) + total).astype(BF16)
            ysnd[t, g] = out
        else:
            scaled, inv, _ = normed_of(source_rows(t, g), g)
            weighted = total * gain[g : g + 1, :]
            inner = jnp.mean(weighted * scaled, axis=-1, keepdims=True)
            upstream = cotf[2 * t + g, me].astype(F32)
            out = (upstream + inv * (weighted - scaled * inner)).astype(BF16)
            dsnd[t, g] = out
            term = total * scaled
            gacc[g] = term if t == 0 else gacc[g] + term
        if t < ticks - 1:
            shift(st, t).start()
        elif st < B0:
            act[g] = out
        else:
            cot[g] = out

    init_items = [(sl, g) for g in range(2) for sl in range(slots)]

    def init_start(i):
        sl, g = init_items[i]
        buf = nsv.at[sl, g]
        buf[me] = normed_of(saved[sl, g].astype(F32), g)[2]
        ag_start(buf, 4 + i)

    def init_relay(i):
        sl, g = init_items[i]
        ag_relay(nsv.at[sl, g], 4 + i)

    def init_finish(i):
        sl, g = init_items[i]
        ag_finish(nsv.at[sl, g], 4 + i)

    def weight_pass(g):
        picked = []
        for t in range(ticks):
            options = [(sl, nsv[sl, g].astype(F32)) for sl in range(slots)]
            options += [(fill[u, g], nrm[2 * u + g].astype(F32)) for u in range(t + 1)]
            picked.append(pick(options, read[t, g]).reshape(tokens, depth).astype(BF16))
        normed = jnp.concatenate(picked, axis=0)
        values = dot_nn(normed, wv[g]).astype(BF16)
        gv[g] = dot_tn(normed, dgs[g]).astype(BF16)
        upstream = jnp.concatenate([whole(cotf, 2 * t + g) for t in range(ticks)], axis=0)
        go[g] = dot_tn(values, upstream).astype(BF16)

    def stash_rows():
        for sl in range(slots):
            for g in range(2):
                rows_now = saved[sl, g].astype(F32)
                for t in range(ticks):
                    rows_now = jnp.where(fill[t, g] == sl, xin[t, g].astype(F32), rows_now)
                stash[sl, g] = rows_now.astype(BF16)

    gain_row = 4 + len(init_items)
    order = (F0, F1, B1, B0)
    pl.semaphore_wait(barrier, 6)
    for st in order:
        stage_s(st, 0)
    for t in range(ticks):
        final = t == ticks - 1
        a, b, c, d = order
        stage_relay(a, t)
        stage_relay(b, t)
        stage_c(a, t)
        stage_relay(c, t)
        stage_c(b, t)
        stage_y(a, t)
        stage_relay(d, t)
        stage_c(c, t)
        if not final:
            init_start(2 * t)
        stage_y(b, t)
        stage_e(a, t)
        stage_c(d, t)
        if not final:
            init_relay(2 * t)
            init_start(2 * t + 1)
        stage_y(c, t)
        stage_e(b, t)
        if not final:
            stage_s(a, t + 1)
            init_relay(2 * t + 1)
        else:
            for i in range(len(init_items)):
                init_finish(i)
            weight_pass(0)
        stage_y(d, t)
        stage_e(c, t)
        if not final:
            stage_s(b, t + 1)
        stage_e(d, t)
        if not final:
            stage_s(c, t + 1)
            stage_s(d, t + 1)
    for g in range(2):
        gsum[me, g : g + 1, :] = jnp.sum(gacc[g], axis=0, keepdims=True)
    ag_start(gsum, gain_row)
    weight_pass(1)
    ag_relay(gsum, gain_row)
    stash_rows()
    ag_finish(gsum, gain_row)
    gg[...] = jnp.sum(gsum[...], axis=0)[0:2, :] * (tokens * ticks) ** (-0.5)
    for st in order:
        ag_drain(buf_of(st, ticks - 1), st)
        for k in range(1, YN):
            rs_y(st, k).wait_send()
        rs_z(st).wait_send()
        for t in range(ticks - 1):
            shift(st, t).wait_send()
    for i, (sl, g) in enumerate(init_items):
        ag_drain(nsv.at[sl, g], 4 + i)
    ag_drain(gsum, gain_row)


def body(n_section, *args):
    w_value, w_out, norm_gain, saved, arriving, returning, fresh, targets, fill, read = args
    wv, wo, gain, saved, arr, ret, fill, read = (
        a[0] for a in (w_value, w_out, norm_gain, saved, arriving, returning, fill, read)
    )
    ticks, rows, depth = fresh.shape
    slots = saved.shape[0]
    feats = wv.shape[2]
    tokens = rows * YN * ZN
    vmem = pl.BlockSpec(memory_space=pltpu.VMEM)
    smem = pl.BlockSpec(memory_space=pltpu.SMEM)
    block = (rows, depth)
    n_rows = 4 + 2 * slots + 1
    dma = pltpu.SemaphoreType.DMA
    outs = pl.pallas_call(
        functools.partial(window, n_section),
        out_shape=(
            jax.ShapeDtypeStruct((2, *block), BF16),
            jax.ShapeDtypeStruct((2, *block), BF16),
            jax.ShapeDtypeStruct((slots, 2, *block), BF16),
            jax.ShapeDtypeStruct(wv.shape, BF16),
            jax.ShapeDtypeStruct(wo.shape, BF16),
            jax.ShapeDtypeStruct((2, depth), F32),
        ),
        in_specs=[vmem] * 8 + [smem] * 2,
        out_specs=[vmem] * 6,
        scratch_shapes=[
            pltpu.VMEM((2 * ticks, 8, *block), BF16),
            pltpu.VMEM((2 * ticks, 8, *block), BF16),
            pltpu.VMEM((slots, 2, 8, *block), BF16),
            pltpu.VMEM((ticks, 2, *block), BF16),
            pltpu.VMEM((4, ZN, YN, *block), BF16),
            pltpu.VMEM((4, YN, ZN, *block), BF16),
            pltpu.VMEM((4, *block), F32),
            pltpu.VMEM((4, *block), BF16),
            pltpu.VMEM((4, *block), BF16),
            pltpu.VMEM((ticks, 2, *block), BF16),
            pltpu.VMEM((ticks, 2, *block), BF16),
            pltpu.VMEM((ticks - 1, 2, *block), BF16),
            pltpu.VMEM((ticks - 1, 2, *block), BF16),
            pltpu.VMEM((2, ticks * tokens, feats), BF16),
            pltpu.VMEM((2, *block), F32),
            pltpu.VMEM((8, 2, depth), F32),
            dma((n_rows, 2 * YN)),
            dma((n_rows, 8)),
            dma((4, YN)),
            dma((4, YN + 1)),
            dma((ticks - 1, 4)),
            dma((ticks - 1, 4)),
        ],
        compiler_params=pltpu.CompilerParams(
            collective_id=0, has_side_effects=True, vmem_limit_bytes=67043328
        ),
        name="window",
    )(wv, wo, gain, saved, arr, ret, fresh, targets, fill, read)
    act, cot, stash, gv, go, gg = outs
    scale = jnp.asarray((ticks * tokens) ** (-0.5), F32)
    gv = (gv.astype(F32) * scale).astype(BF16)
    go = (go.astype(F32) * scale).astype(BF16)
    return tuple(a[None] for a in (act, cot, stash, gv, go, gg))


def solution(mesh):
    in_specs = (
        P("section", None, None, "dp"),
        P("section", None, "dp", None),
        P("section", None, None),
        P("section", None, None, "dp", None),
        P("section", None, "dp", None),
        P("section", None, "dp", None),
        P(None, "dp", None),
        P(None, "dp", None),
        P("section", None, None),
        P("section", None, None),
    )
    out_specs = (
        P("section", None, "dp", None),
        P("section", None, "dp", None),
        P("section", None, None, "dp", None),
        P("section", None, None, "dp"),
        P("section", None, "dp", None),
        P("section", None, None),
    )
    return jax.shard_map(
        functools.partial(body, mesh.shape["section"]),
        mesh=mesh,
        in_specs=in_specs,
        out_specs=out_specs,
        check_vma=False,
    )
```

```python
import functools

import jax
import jax.numpy as jnp
from jax import lax
from jax.experimental import pallas as pl
from jax.experimental.pallas import tpu as pltpu
from jax.sharding import PartitionSpec as P

epsilon = 1e-06
MESH = pl.DeviceIdType.MESH
F32, BF16 = jnp.float32, jnp.bfloat16

F0, F1, B0, B1 = range(4)
YN, ZN = 4, 2

PIECES = {
    "y1": ((0, 0, None), 1),
    "y3": ((0, 0, None), -1),
    "y2": ((0, 0, None), 2),
    "z0": ((0, 0, None), "z"),
    "z1": ((0, -1, None), "z"),
    "z3": ((0, 1, None), "z"),
    "z2": ((0, 2, None), "z"),
    "w1": ((1, 0, None), 1),
    "w3": ((1, 0, None), -1),
    "h1": ((0, -1, 0), 1),
    "h3": ((0, 1, 1), -1),
    "v1": ((1, -1, 0), 1),
    "v3": ((1, 1, 1), -1),
}
GATHERS = {
    "Y": {
        "S": ((), ("y2", "y1", "y3", "z0")),
        "R": (("y1", "y3", "y2"), ("z1", "z3", "z2")),
        "C": (("z0", "z1", "z3", "z2"), ()),
    },
    "YR": {
        "S": ((), ("y1", "y3", "z0")),
        "R": (("y1", "y3"), ("h1", "h3", "z1", "z3")),
        "Q": (("h1", "h3"), ("z2",)),
        "C": (("z0", "z1", "z3", "z2"), ()),
    },
    "ZR": {
        "S": ((), ("z0", "y1", "y3")),
        "R": (("z0", "y1", "y3"), ("w1", "w3", "h1", "h3")),
        "Q": (("w1", "w3"), ("v1", "v3")),
        "C": (("h1", "h3", "v1", "v3"), ()),
    },
}
N_KEYS = 9
STREAM_MODES = (("YR", "yr"), ("ZR", "zr"), ("ZR", "zr"), ("YR", "yr"))
INIT_MODE = "ZR"
ORDER = (
    "S20", "S10", "S00", "S30", "R00", "R10", "R20", "Q00", "R30", "Q10", "Q20", "C00",
    "Q30", "S50", "C10", "C30", "P00", "C20", "Y00", "R50", "P30", "S90", "P20", "P10",
    "E00", "S40", "Y10", "Y30", "S01", "Y20", "E30", "E10", "R40", "R01", "Q50", "E20",
    "S11", "Q01", "S31", "R11", "S21", "R31", "Q11", "R21", "Q31", "C01", "C11", "Q21",
    "C31", "C21", "Q40", "P31", "P01", "P11", "Y31", "Y01", "P21", "Y11", "E31", "R90",
    "E01", "Y21", "S80", "E11", "S32", "S02", "E21", "S12", "R32", "S22", "Q32", "R12",
    "R02", "Q12", "R22", "C32", "Q02", "C12", "Q22", "P32", "Q90", "C22", "C02", "Y32",
    "S60", "P12", "P02", "S70", "P22", "Y02", "Y12", "Y22", "R80", "E32", "R70", "E02",
    "E22", "E12", "S33", "S03", "S23", "S13", "R03", "R23", "R33", "Q23", "R13", "Q80",
    "R60", "Q33", "C23", "Q70", "T00", "C33", "Q03", "Q13", "Q60", "P33", "C13", "P23",
    "C03", "Y23", "P03", "Y33", "W10", "P13", "E23", "E33", "G00", "W00", "Y03", "Y13",
    "H00", "E13", "E03",
)
VMEM_LIMIT = 52428800


def scoped(stage):
    def run(*ids):
        with jax.named_scope("_".join([stage.__name__] + [str(i) for i in ids])):
            return stage(*ids)

    return run


def dot_nn(a, b):
    return jnp.dot(a, b, preferred_element_type=F32)


def dot_nt(a, b):
    return lax.dot_general(a, b, (((1,), (1,)), ((), ())), preferred_element_type=F32)


def dot_tn(a, b):
    return lax.dot_general(a, b, (((0,), (0,)), ((), ())), preferred_element_type=F32)


def window(
    n_section,
    gain, arr, ret, wv_in, wo_in, saved_in, fresh_in, tgt_in, fill, read,
    act, cot, stash, gv, go, gg,
    wv, wo, saved, fresh, tgt,
    nrm, cotf, nsv, xin, part, rsh, rsy, zq, keep, zs, zr, ysnd, dsnd, shf, shb, dgs, gacc, gsum,
    in_s, ag_s, ag_r, rs_s, rs_r, sh_s, sh_r, g_s, g_r,
):
    ticks = fresh.shape[0]
    slots = saved.shape[0]
    depth = gain.shape[1]
    half = depth // 2
    rows = arr.shape[1]
    tokens = rows * YN * ZN
    me = lax.axis_index("dp")
    sec = lax.axis_index("section")
    z, y = me // YN, me % YN
    zp = 1 - z
    first = sec == 0
    last = sec == n_section - 1
    nxt = lax.rem(sec + 1, n_section)
    prv = lax.rem(sec + n_section - 1, n_section)

    def y_at(k):
        return lax.rem(y + k + YN, YN)

    def to(where):
        if where == "z":
            return {"dp": zp * YN + y}
        return {"dp": z * YN + y_at(where)}

    others = [(dz, dy) for dz in range(ZN) for dy in range(YN) if dz or dy]

    def other(dz, dy):
        return (zp if dz else z) * YN + y_at(dy)

    barrier = pltpu.get_barrier_semaphore()
    for target in [{"dp": other(*o)} for o in others] + [{"section": nxt}, {"section": prv}]:
        pl.semaphore_signal(barrier, inc=1, device_id=target, device_id_type=MESH)

    loads = {
        "wv": (wv_in, wv),
        "wo": (wo_in, wo),
        "saved": (saved_in, saved),
        "fresh": (fresh_in, fresh),
        "tgt": (tgt_in, tgt),
    }
    loads = {
        name: pltpu.make_async_copy(src, dst, in_s.at[i]) for i, (name, (src, dst)) in enumerate(loads.items())
    }
    for copy in loads.values():
        copy.start()
    loaded = set()

    def need(*names):
        for name in names:
            if name not in loaded:
                loads[name].wait()
                loaded.add(name)

    def send(src, dst, s, r, target):
        return pltpu.make_async_remote_copy(
            src_ref=src, dst_ref=dst, send_sem=s, recv_sem=r, device_id=target, device_id_type=MESH
        )

    def columns(h):
        return pl.ds(0, depth) if h is None else pl.ds(h * half, half)

    init_items = [(sl, g) for g in range(2) for sl in range(slots)]

    def mode_of(row):
        return STREAM_MODES[row][0] if row < 4 else INIT_MODE

    def buf_of(row, t):
        if row >= 4:
            return nsv.at[init_items[row - 4]]
        return (nrm if row < B0 else cotf).at[2 * t + row % 2]

    def gather_copy(row, t, key, arriving=False):
        (dz, dy, h), where = PIECES[key]
        if arriving:
            dz, dy = (1 - dz, dy) if where == "z" else (dz, dy - where)
        block = buf_of(row, t).at[other(dz, dy), :, columns(h)]
        i = [k for _, sends in GATHERS[mode_of(row)].values() for k in sends].index(key)
        return send(block, block, ag_s.at[row, i], ag_r.at[row, i], to(where))

    def gather(stage, row, t):
        waits, sends = GATHERS[mode_of(row)][stage]
        for key in waits:
            gather_copy(row, t, key, arriving=True).wait_recv()
        for key in sends:
            gather_copy(row, t, key).start()

    def gather_drain(row, t):
        for _, sends in GATHERS[mode_of(row)].values():
            for key in sends:
                gather_copy(row, t, key).wait_send()

    def sum_copy(st, key):
        i = ("h1", "h3", "p1", "p3", "q").index(key)
        over_y = STREAM_MODES[st][1] == "yr"
        if key == "q":
            src, dst = (zs.at[st], zr.at[st]) if over_y else (part.at[st, zp], zq.at[st])
            return send(src, dst, rs_s.at[st, i], rs_r.at[st, i], to("z"))
        zz = pl.ds(0, ZN) if over_y else pl.ds(z, 1)
        way = 1 if key[1] == "1" else -1
        side = 0 if way == 1 else 1
        if key[0] == "h":
            src = part.at[st, zz, y_at(2), :, columns(side)]
            dst = rsh.at[st, side, pl.ds(0, ZN if over_y else 1)]
        else:
            src = part.at[st, zz, y_at(way)]
            dst = rsy.at[st, side, pl.ds(0, ZN if over_y else 1)]
        return send(src, dst, rs_s.at[st, i], rs_r.at[st, i], to(way))

    def sum_wait(st, *keys):
        for key in keys:
            sum_copy(st, key).wait_recv()

    def sum_start(st, *keys):
        for key in keys:
            sum_copy(st, key).start()

    def sum_drain(st):
        for key in ("h1", "h3", "p1", "p3", "q"):
            sum_copy(st, key).wait_send()

    def add_halves(st, zz, slot):
        for side, way in ((0, 1), (1, -1)):
            at = (st, zz, y_at(way), slice(None), columns(side))
            part[at] = (part[at].astype(F32) + rsh[st, side, slot].astype(F32)).astype(BF16)

    def shift(st, t):
        g = st % 2
        if st < B0:
            return send(ysnd.at[t, g], shf.at[t, g], sh_s.at[t, st], sh_r.at[t, st], {"section": nxt})
        return send(dsnd.at[t, g], shb.at[t, g], sh_s.at[t, st], sh_r.at[t, st], {"section": prv})

    def normed_of(x, g):
        inv = lax.rsqrt(jnp.mean(x * x, axis=-1, keepdims=True) + epsilon)
        scaled = x * inv
        return scaled, inv, (scaled * gain[g : g + 1, :]).astype(BF16)

    def whole(ref, i):
        return ref[i].astype(F32).reshape(tokens, depth).astype(BF16)

    @scoped
    def stage_s(st, t):
        if st >= 4:
            need("saved")
            sl, g = init_items[st - 4]
            buf_of(st, t)[me] = normed_of(saved[sl, g].astype(F32), g)[2]
            gather("S", st, t)
            return
        g = st % 2
        if t > 0:
            shift(st, t - 1).wait_recv()
        if st < B0:
            if t == 0:
                x = arr[g].astype(F32)
            else:
                need("fresh")
                edge = fresh[t] if g == 0 else shf[t - 1, 0]
                x = jnp.where(first, edge.astype(F32), shf[t - 1, g].astype(F32))
            xin[t, g] = x.astype(BF16)
            own = normed_of(x, g)[2]
        elif t == 0:
            own = ret[g]
        else:
            if g == 0:
                edge = shb[t - 1, 1].astype(F32)
            else:
                need("tgt")
                edge = ysnd[t - 1, 1].astype(F32) - tgt[t - 1].astype(F32)
            own = jnp.where(last, edge, shb[t - 1, g].astype(F32)).astype(BF16)
        if t > 0:
            gather_drain(st, t - 1)
        buf_of(st, t)[me] = own
        gather("S", st, t)

    @scoped
    def stage_r(row, t):
        gather("R", row, t)

    @scoped
    def stage_q(row, t):
        gather("Q", row, t)

    @scoped
    def stage_c(st, t):
        g = st % 2
        gather("C", st, t)
        need("wv", "wo")
        if st < B0:
            values = dot_nn(whole(nrm, 2 * t + g), wv[g]).astype(BF16)
            terms = dot_nn(values, wo[g])
        else:
            down = dot_nt(whole(cotf, 2 * t + g), wo[g]).astype(BF16)
            dgs[g, t * tokens : (t + 1) * tokens, :] = down
            terms = dot_nt(down, wv[g])
        if t > 0:
            sum_drain(st)
        part[st] = terms.reshape(ZN, YN, rows, depth).astype(BF16)
        if STREAM_MODES[st][1] == "yr":
            sum_start(st, "h1", "h3")
        else:
            sum_start(st, "q")

    @scoped
    def stage_p(st, t):
        if STREAM_MODES[st][1] == "yr":
            sum_wait(st, "h1", "h3")
            for zz in range(ZN):
                add_halves(st, zz, zz)
            sum_start(st, "p1", "p3")
        else:
            sum_wait(st, "q")
            for k in (2, 1, 3, 0):
                both = part[st, z, y_at(k)].astype(F32) + zq[st, y_at(k)].astype(F32)
                if k:
                    part[st, z, y_at(k)] = both.astype(BF16)
                else:
                    keep[st] = both
                if k == 2:
                    sum_start(st, "h1", "h3")

    @scoped
    def stage_y(st, t):
        if STREAM_MODES[st][1] == "yr":
            sum_wait(st, "p1", "p3")

            def total(zz):
                acc = part[st, zz, y].astype(F32) + rsy[st, 0, zz].astype(F32)
                return acc + rsy[st, 1, zz].astype(F32)

            zs[st] = total(zp).astype(BF16)
            sum_start(st, "q")
            keep[st] = total(z)
        else:
            sum_wait(st, "h1", "h3")
            add_halves(st, z, 0)
            sum_start(st, "p1", "p3")

    def pick(candidates, which):
        chosen = candidates[0][1]
        for index, value in candidates[1:]:
            chosen = jnp.where(index == which, value, chosen)
        return chosen

    def source_rows(t, g):
        options = [(sl, saved[sl, g].astype(F32)) for sl in range(slots)]
        options += [(fill[0, u, g], xin[u, g].astype(F32)) for u in range(t + 1)]
        return pick(options, read[0, t, g])

    @scoped
    def stage_e(st, t):
        g = st % 2
        if STREAM_MODES[st][1] == "yr":
            sum_wait(st, "q")
            total = keep[st] + zr[st].astype(F32)
        else:
            sum_wait(st, "p1", "p3")
            total = keep[st] + rsy[st, 0, 0].astype(F32) + rsy[st, 1, 0].astype(F32)
        if st < B0:
            out = (xin[t, g].astype(F32) + total).astype(BF16)
            ysnd[t, g] = out
        else:
            need("saved")
            scaled, inv, _ = normed_of(source_rows(t, g), g)
            weighted = total * gain[g : g + 1, :]
            inner = jnp.mean(weighted * scaled, axis=-1, keepdims=True)
            upstream = cotf[2 * t + g, me].astype(F32)
            out = (upstream + inv * (weighted - scaled * inner)).astype(BF16)
            dsnd[t, g] = out
            term = total * scaled
            gacc[g] = term if t == 0 else gacc[g] + term
        if t < ticks - 1:
            shift(st, t).start()
        elif st < B0:
            act[g] = out
        else:
            cot[g] = out

    @scoped
    def stage_w(g, _):
        for i in range(slots):
            gather("C", 4 + g * slots + i, 0)
        picked = []
        for t in range(ticks):
            options = [(sl, nsv[sl, g].astype(F32)) for sl in range(slots)]
            options += [(fill[0, u, g], nrm[2 * u + g].astype(F32)) for u in range(t + 1)]
            picked.append(pick(options, read[0, t, g]).reshape(tokens, depth).astype(BF16))
        normed = jnp.concatenate(picked, axis=0)
        values = dot_nn(normed, wv[g]).astype(BF16)
        gv[g] = dot_tn(normed, dgs[g]).astype(BF16)
        upstream = jnp.concatenate([whole(cotf, 2 * t + g) for t in range(ticks)], axis=0)
        go[g] = dot_tn(values, upstream).astype(BF16)

    @scoped
    def stage_t(_, __):
        for sl in range(slots):
            for g in range(2):
                rows_now = saved[sl, g].astype(F32)
                for t in range(ticks):
                    rows_now = jnp.where(fill[0, t, g] == sl, xin[t, g].astype(F32), rows_now)
                stash[sl, g] = rows_now.astype(BF16)

    def gain_copy(i, arriving=False):
        peer = other(*others[i])
        row = peer if arriving else me
        return send(gsum.at[row], gsum.at[row], g_s.at[i], g_r.at[i], {"dp": peer})

    @scoped
    def stage_g(_, __):
        for g in range(2):
            gsum[me, g : g + 1, :] = jnp.sum(gacc[g], axis=0, keepdims=True)
        for i in range(len(others)):
            gain_copy(i).start()

    @scoped
    def stage_h(_, __):
        for i, (dz, dy) in enumerate(others):
            j = others.index((dz, -dy % YN))
            peer = other(dz, dy)
            send(gsum.at[peer], gsum.at[peer], g_s.at[j], g_r.at[j], {"dp": peer}).wait_recv()
        gg[...] = jnp.sum(gsum[...], axis=0) * (tokens * ticks) ** (-0.5)

    pl.semaphore_wait(barrier, len(others) + 2)
    stages = {
        "S": stage_s, "R": stage_r, "Q": stage_q, "C": stage_c, "P": stage_p, "Y": stage_y,
        "E": stage_e, "W": stage_w, "T": stage_t, "G": stage_g, "H": stage_h,
    }
    for step in ORDER:
        stages[step[0]](int(step[1]), int(step[2]))
    for st in range(4):
        gather_drain(st, ticks - 1)
        sum_drain(st)
        for t in range(ticks - 1):
            shift(st, t).wait_send()
    for i in range(len(init_items)):
        gather_drain(4 + i, 0)
    for i in range(len(others)):
        gain_copy(i).wait_send()


def body(n_section, *args):
    w_value, w_out, norm_gain, saved, arriving, returning, fresh, targets, fill, read = args
    wv, wo, gain, saved, arr, ret = (
        a[0] for a in (w_value, w_out, norm_gain, saved, arriving, returning)
    )
    ticks, rows, depth = fresh.shape
    slots = saved.shape[0]
    feats = wv.shape[2]
    tokens = rows * YN * ZN
    vmem = pl.BlockSpec(memory_space=pltpu.VMEM)
    smem = pl.BlockSpec(memory_space=pltpu.SMEM)
    hbm = pl.BlockSpec(memory_space=pltpu.HBM)
    block = (rows, depth)
    n_rows = 4 + 2 * slots
    dma = pltpu.SemaphoreType.DMA
    held = [pltpu.VMEM(a.shape, a.dtype) for a in (wv, wo, saved, fresh, targets)]
    outs = pl.pallas_call(
        functools.partial(window, n_section),
        out_shape=(
            jax.ShapeDtypeStruct((2, *block), BF16),
            jax.ShapeDtypeStruct((2, *block), BF16),
            jax.ShapeDtypeStruct((slots, 2, *block), BF16),
            jax.ShapeDtypeStruct(wv.shape, BF16),
            jax.ShapeDtypeStruct(wo.shape, BF16),
            jax.ShapeDtypeStruct((2, depth), F32),
        ),
        in_specs=[vmem] * 3 + [hbm] * 5 + [smem] * 2,
        out_specs=[vmem] * 6,
        scratch_shapes=held
        + [
            pltpu.VMEM((2 * ticks, 8, *block), BF16),
            pltpu.VMEM((2 * ticks, 8, *block), BF16),
            pltpu.VMEM((slots, 2, 8, *block), BF16),
            pltpu.VMEM((ticks, 2, *block), BF16),
            pltpu.VMEM((4, ZN, YN, *block), BF16),
            pltpu.VMEM((4, 2, ZN, rows, depth // 2), BF16),
            pltpu.VMEM((4, 2, ZN, *block), BF16),
            pltpu.VMEM((4, YN, *block), BF16),
            pltpu.VMEM((4, *block), F32),
            pltpu.VMEM((4, *block), BF16),
            pltpu.VMEM((4, *block), BF16),
            pltpu.VMEM((ticks, 2, *block), BF16),
            pltpu.VMEM((ticks, 2, *block), BF16),
            pltpu.VMEM((ticks - 1, 2, *block), BF16),
            pltpu.VMEM((ticks - 1, 2, *block), BF16),
            pltpu.VMEM((2, ticks * tokens, feats), BF16),
            pltpu.VMEM((2, *block), F32),
            pltpu.VMEM((8, 2, depth), F32),
            dma((len(held),)),
            dma((n_rows, N_KEYS)),
            dma((n_rows, N_KEYS)),
            dma((4, 5)),
            dma((4, 5)),
            dma((ticks - 1, 4)),
            dma((ticks - 1, 4)),
            dma((7,)),
            dma((7,)),
        ],
        compiler_params=pltpu.CompilerParams(
            collective_id=0, has_side_effects=True, vmem_limit_bytes=VMEM_LIMIT
        ),
        name="window",
    )(gain, arr, ret, wv, wo, saved, fresh, targets, fill, read)
    act, cot, stash, gv, go, gg = outs
    scale = jnp.asarray((ticks * tokens) ** (-0.5), F32)
    gv = (gv.astype(F32) * scale).astype(BF16)
    go = (go.astype(F32) * scale).astype(BF16)
    return tuple(a[None] for a in (act, cot, stash, gv, go, gg))


def solution(mesh):
    in_specs = (
        P("section", None, None, "dp"),
        P("section", None, "dp", None),
        P("section", None, None),
        P("section", None, None, "dp", None),
        P("section", None, "dp", None),
        P("section", None, "dp", None),
        P(None, "dp", None),
        P(None, "dp", None),
        P("section", None, None),
        P("section", None, None),
    )
    out_specs = (
        P("section", None, "dp", None),
        P("section", None, "dp", None),
        P("section", None, None, "dp", None),
        P("section", None, None, "dp"),
        P("section", None, "dp", None),
        P("section", None, None),
    )
    return jax.shard_map(
        functools.partial(body, mesh.shape["section"]),
        mesh=mesh,
        in_specs=in_specs,
        out_specs=out_specs,
        check_vma=False,
    )
```

```python
import functools

import jax
import jax.numpy as jnp
from jax import lax
from jax.experimental import pallas as pl
from jax.experimental.pallas import tpu as pltpu
from jax.sharding import PartitionSpec as P

epsilon = 1e-06
MESH = pl.DeviceIdType.MESH
F32, BF16 = jnp.float32, jnp.bfloat16

F0, F1, B0, B1 = range(4)
YN, ZN = 4, 2

PIECES = {
    "y1": ((0, 0, None), 1),
    "y3": ((0, 0, None), -1),
    "z0": ((0, 0, None), "z"),
    "z1": ((0, -1, None), "z"),
    "z3": ((0, 1, None), "z"),
    "z2": ((0, 2, None), "z"),
    "w1": ((1, 0, None), 1),
    "w3": ((1, 0, None), -1),
    "h1": ((0, -1, 0), 1),
    "h3": ((0, 1, 1), -1),
    "v1": ((1, -1, 0), 1),
    "v3": ((1, 1, 1), -1),
}
KEYS = tuple(PIECES)
GATHERS = {
    "Y": {
        "S": ((), ("y1", "y3", "z0")),
        "R": (("y1", "y3"), ("h1", "h3", "z1", "z3")),
        "Q": (("h1", "h3"), ("z2",)),
        "C": (("z0", "z1", "z3", "z2"), ()),
    },
    "Z": {
        "S": ((), ("z0", "y1", "y3")),
        "R": (("z0", "y1", "y3"), ("w1", "w3", "h1", "h3")),
        "Q": (("w1", "w3"), ("v1", "v3")),
        "C": (("h1", "h3", "v1", "v3"), ()),
    },
}
STREAM_GATHERS = ("YZZY", "ZYYY", "ZYZY", "YZYZ")
STREAM_SUMS = ("YYYZ", "YYYY", "ZYZY", "YZYY")
INIT_GATHERS = "ZYZZYZ"
ORDER = (
    "S00", "S10", "S20", "R00", "S30", "R10", "R20", "Q00", "R30", "Q10", "Q20", "C00",
    "S80", "Q30", "C10", "C20", "P00", "C30", "P10", "Y00", "P30", "P20", "S50", "E00",
    "S60", "Y10", "Y30", "Y20", "S01", "E10", "E30", "S70", "E20", "S40", "R01", "S11",
    "S31", "S21", "R11", "Q01", "R31", "Q11", "R21", "Q31", "C01", "Q21", "C11", "C31",
    "P01", "C21", "P11", "Y01", "R50", "P31", "P21", "E01", "Y31", "R60", "Y11", "Y21",
    "E31", "S02", "R70", "E21", "E11", "R80", "R02", "S32", "S22", "S12", "R32", "Q02",
    "R22", "Q32", "R12", "C02", "Q22", "R40", "Q12", "C32", "P02", "C22", "C12", "P32",
    "S90", "P22", "Y02", "P12", "Y32", "E02", "Q50", "Y22", "Q40", "E32", "R90", "Y12",
    "E22", "S03", "Q60", "E12", "S33", "R03", "S23", "R33", "R23", "Q33", "Q70", "Q23",
    "S13", "Q03", "C33", "R13", "C23", "P33", "Q13", "C03", "P23", "C13", "W00", "Y33",
    "Q90", "Y23", "P13", "P03", "E33", "Q80", "E23", "G00", "Y03", "Y13", "W10", "T00",
    "H00", "E13", "E03",
)
VMEM_LIMIT = 67043328


def scoped(stage):
    def run(*ids):
        with jax.named_scope("_".join([stage.__name__] + [str(i) for i in ids])):
            return stage(*ids)

    return run


def dot_nn(a, b):
    return jnp.dot(a, b, preferred_element_type=F32)


def dot_nt(a, b):
    return lax.dot_general(a, b, (((1,), (1,)), ((), ())), preferred_element_type=F32)


def dot_tn(a, b):
    return lax.dot_general(a, b, (((0,), (0,)), ((), ())), preferred_element_type=F32)


def window(
    n_section,
    gain, arr, ret, wv_in, wo_in, saved_in, fresh_in, tgt_in, fill, read,
    act_out, cot_out, stash_out, gv_out, go_out, gg_out,
    act, cot, stash, gv, go, gg,
    wv, wo, saved, fresh, tgt,
    nrm, cotf, nsv, xin, part, rsh, rsy, zq, keep, zs, zr, ysnd, dsnd, shf, shb, dgs, gacc, gsum,
    in_s, out_s, ag_s, ag_r, rs_s, rs_r, sh_s, sh_r, g_s, g_r,
):
    ticks = fresh.shape[0]
    slots = saved.shape[0]
    depth = gain.shape[1]
    half = depth // 2
    rows = arr.shape[1]
    tokens = rows * YN * ZN
    scale = (tokens * ticks) ** (-0.5)
    me = lax.axis_index("dp")
    sec = lax.axis_index("section")
    z, y = me // YN, me % YN
    zp = 1 - z
    first = sec == 0
    last = sec == n_section - 1
    nxt = lax.rem(sec + 1, n_section)
    prv = lax.rem(sec + n_section - 1, n_section)

    def y_at(k):
        return lax.rem(y + k + YN, YN)

    def to(where):
        if where == "z":
            return {"dp": zp * YN + y}
        return {"dp": z * YN + y_at(where)}

    others = [(dz, dy) for dz in range(ZN) for dy in range(YN) if dz or dy]

    def other(dz, dy):
        return (zp if dz else z) * YN + y_at(dy)

    barrier = pltpu.get_barrier_semaphore()
    for target in [{"dp": other(*o)} for o in others] + [{"section": nxt}, {"section": prv}]:
        pl.semaphore_signal(barrier, inc=1, device_id=target, device_id_type=MESH)

    loads = {
        "wv": (wv_in, wv),
        "wo": (wo_in, wo),
        "saved": (saved_in, saved),
        "fresh": (fresh_in, fresh),
        "tgt": (tgt_in, tgt),
    }
    loads = {
        name: pltpu.make_async_copy(src, dst, in_s.at[i]) for i, (name, (src, dst)) in enumerate(loads.items())
    }
    for copy in loads.values():
        copy.start()
    loaded = set()

    def need(*names):
        for name in names:
            if name not in loaded:
                loads[name].wait()
                loaded.add(name)

    results = []

    def put(src, dst):
        copy = pltpu.make_async_copy(src, dst, out_s.at[len(results)])
        results.append(copy)
        copy.start()

    def send(src, dst, s, r, target):
        return pltpu.make_async_remote_copy(
            src_ref=src, dst_ref=dst, send_sem=s, recv_sem=r, device_id=target, device_id_type=MESH
        )

    def columns(h):
        return pl.ds(0, depth) if h is None else pl.ds(h * half, half)

    init_items = [(sl, g) for g in range(2) for sl in range(slots)]

    def mode_of(row, t):
        return STREAM_GATHERS[row][t] if row < 4 else INIT_GATHERS[row - 4]

    def over_y(st, t):
        return STREAM_SUMS[st][t] == "Y"

    def buf_of(row, t):
        if row >= 4:
            return nsv.at[init_items[row - 4]]
        return (nrm if row < B0 else cotf).at[2 * t + row % 2]

    def gather_copy(row, t, key, arriving=False):
        (dz, dy, h), where = PIECES[key]
        if arriving:
            dz, dy = (1 - dz, dy) if where == "z" else (dz, dy - where)
        block = buf_of(row, t).at[other(dz, dy), :, columns(h)]
        i = KEYS.index(key)
        return send(block, block, ag_s.at[row, i], ag_r.at[row, i], to(where))

    def gather(stage, row, t):
        waits, sends = GATHERS[mode_of(row, t)][stage]
        for key in waits:
            gather_copy(row, t, key, arriving=True).wait_recv()
        for key in sends:
            gather_copy(row, t, key).start()

    def gather_drain(row, t):
        for _, sends in GATHERS[mode_of(row, t)].values():
            for key in sends:
                gather_copy(row, t, key).wait_send()

    def sum_copy(st, t, key):
        i = ("h1", "h3", "p1", "p3", "q").index(key)
        n = ZN if over_y(st, t) else 1
        if key == "q":
            src, dst = (zs.at[st], zr.at[st]) if over_y(st, t) else (part.at[st, zp], zq.at[st])
            return send(src, dst, rs_s.at[st, i], rs_r.at[st, i], to("z"))
        zz = pl.ds(0 if over_y(st, t) else z, n)
        way = 1 if key[1] == "1" else -1
        side = 0 if way == 1 else 1
        if key[0] == "h":
            src = part.at[st, zz, y_at(2), :, columns(side)]
            dst = rsh.at[st, side, pl.ds(0, n)]
        else:
            src = part.at[st, zz, y_at(way)]
            dst = rsy.at[st, side, pl.ds(0, n)]
        return send(src, dst, rs_s.at[st, i], rs_r.at[st, i], to(way))

    def sum_wait(st, t, *keys):
        for key in keys:
            sum_copy(st, t, key).wait_recv()

    def sum_start(st, t, *keys):
        for key in keys:
            sum_copy(st, t, key).start()

    def sum_drain(st, t):
        for key in ("h1", "h3", "p1", "p3", "q"):
            sum_copy(st, t, key).wait_send()

    def add_halves(st, zz, slot):
        for side, way in ((0, 1), (1, -1)):
            at = (st, zz, y_at(way), slice(None), columns(side))
            part[at] = (part[at].astype(F32) + rsh[st, side, slot].astype(F32)).astype(BF16)

    def shift(st, t):
        g = st % 2
        if st < B0:
            return send(ysnd.at[t, g], shf.at[t, g], sh_s.at[t, st], sh_r.at[t, st], {"section": nxt})
        return send(dsnd.at[t, g], shb.at[t, g], sh_s.at[t, st], sh_r.at[t, st], {"section": prv})

    def normed_of(x, g):
        inv = lax.rsqrt(jnp.mean(x * x, axis=-1, keepdims=True) + epsilon)
        scaled = x * inv
        return scaled, inv, (scaled * gain[g : g + 1, :]).astype(BF16)

    def whole(ref, i):
        return ref[i].astype(F32).reshape(tokens, depth).astype(BF16)

    @scoped
    def stage_s(st, t):
        if st >= 4:
            need("saved")
            sl, g = init_items[st - 4]
            buf_of(st, t)[me] = normed_of(saved[sl, g].astype(F32), g)[2]
            gather("S", st, t)
            return
        g = st % 2
        if t > 0:
            shift(st, t - 1).wait_recv()
        if st < B0:
            if t == 0:
                x = arr[g].astype(F32)
            else:
                need("fresh")
                edge = fresh[t] if g == 0 else shf[t - 1, 0]
                x = jnp.where(first, edge.astype(F32), shf[t - 1, g].astype(F32))
            xin[t, g] = x.astype(BF16)
            own = normed_of(x, g)[2]
        elif t == 0:
            own = ret[g]
        else:
            if g == 0:
                edge = shb[t - 1, 1].astype(F32)
            else:
                need("tgt")
                edge = ysnd[t - 1, 1].astype(F32) - tgt[t - 1].astype(F32)
            own = jnp.where(last, edge, shb[t - 1, g].astype(F32)).astype(BF16)
        if t > 0:
            gather_drain(st, t - 1)
        buf_of(st, t)[me] = own
        gather("S", st, t)

    @scoped
    def stage_r(row, t):
        gather("R", row, t)

    @scoped
    def stage_q(row, t):
        gather("Q", row, t)

    @scoped
    def stage_c(st, t):
        g = st % 2
        gather("C", st, t)
        need("wv", "wo")
        if st < B0:
            values = dot_nn(whole(nrm, 2 * t + g), wv[g]).astype(BF16)
            terms = dot_nn(values, wo[g])
        else:
            down = dot_nt(whole(cotf, 2 * t + g), wo[g]).astype(BF16)
            dgs[g, t * tokens : (t + 1) * tokens, :] = down
            terms = dot_nt(down, wv[g])
        if t > 0:
            sum_drain(st, t - 1)
        part[st] = terms.reshape(ZN, YN, rows, depth).astype(BF16)
        if over_y(st, t):
            sum_start(st, t, "h1", "h3")
        else:
            sum_start(st, t, "q")

    @scoped
    def stage_p(st, t):
        if over_y(st, t):
            sum_wait(st, t, "h1", "h3")
            for zz in range(ZN):
                add_halves(st, zz, zz)
            sum_start(st, t, "p1", "p3")
        else:
            sum_wait(st, t, "q")
            for k in (2, 1, 3, 0):
                both = part[st, z, y_at(k)].astype(F32) + zq[st, y_at(k)].astype(F32)
                if k:
                    part[st, z, y_at(k)] = both.astype(BF16)
                else:
                    keep[st] = both
                if k == 2:
                    sum_start(st, t, "h1", "h3")

    @scoped
    def stage_y(st, t):
        if over_y(st, t):
            sum_wait(st, t, "p1", "p3")

            def total(zz):
                acc = part[st, zz, y].astype(F32) + rsy[st, 0, zz].astype(F32)
                return acc + rsy[st, 1, zz].astype(F32)

            zs[st] = total(zp).astype(BF16)
            sum_start(st, t, "q")
            keep[st] = total(z)
        else:
            sum_wait(st, t, "h1", "h3")
            add_halves(st, z, 0)
            sum_start(st, t, "p1", "p3")

    def pick(candidates, which):
        chosen = candidates[0][1]
        for index, value in candidates[1:]:
            chosen = jnp.where(index == which, value, chosen)
        return chosen

    def source_rows(t, g):
        options = [(sl, saved[sl, g].astype(F32)) for sl in range(slots)]
        options += [(fill[0, g, u], xin[u, g].astype(F32)) for u in range(t + 1)]
        return pick(options, read[0, g, t])

    @scoped
    def stage_e(st, t):
        g = st % 2
        if over_y(st, t):
            sum_wait(st, t, "q")
            total = keep[st] + zr[st].astype(F32)
        else:
            sum_wait(st, t, "p1", "p3")
            total = keep[st] + rsy[st, 0, 0].astype(F32) + rsy[st, 1, 0].astype(F32)
        if st < B0:
            out = (xin[t, g].astype(F32) + total).astype(BF16)
            ysnd[t, g] = out
        else:
            need("saved")
            scaled, inv, _ = normed_of(source_rows(t, g), g)
            weighted = total * gain[g : g + 1, :]
            inner = jnp.mean(weighted * scaled, axis=-1, keepdims=True)
            upstream = cotf[2 * t + g, me].astype(F32)
            out = (upstream + inv * (weighted - scaled * inner)).astype(BF16)
            dsnd[t, g] = out
            term = total * scaled
            gacc[g] = term if t == 0 else gacc[g] + term
        if t < ticks - 1:
            shift(st, t).start()
        elif st < B0:
            act[g] = out
            put(act.at[g], act_out.at[g])
        else:
            cot[g] = out
            put(cot.at[g], cot_out.at[g])

    @scoped
    def stage_w(g, _):
        for i in range(slots):
            gather("C", 4 + g * slots + i, 0)
        picked = []
        for t in range(ticks):
            options = [(sl, nsv[sl, g].astype(F32)) for sl in range(slots)]
            options += [(fill[0, g, u], nrm[2 * u + g].astype(F32)) for u in range(t + 1)]
            picked.append(pick(options, read[0, g, t]).reshape(tokens, depth).astype(BF16))
        normed = jnp.concatenate(picked, axis=0)
        values = dot_nn(normed, wv[g]).astype(BF16)
        gv[g] = (dot_tn(normed, dgs[g]) * scale).astype(BF16)
        put(gv.at[g], gv_out.at[g])
        upstream = jnp.concatenate([whole(cotf, 2 * t + g) for t in range(ticks)], axis=0)
        go[g] = (dot_tn(values, upstream) * scale).astype(BF16)
        put(go.at[g], go_out.at[g])

    @scoped
    def stage_t(_, __):
        for sl in range(slots):
            for g in range(2):
                rows_now = saved[sl, g].astype(F32)
                for t in range(ticks):
                    rows_now = jnp.where(fill[0, g, t] == sl, xin[t, g].astype(F32), rows_now)
                stash[sl, g] = rows_now.astype(BF16)
        put(stash, stash_out)

    def gain_copy(i, arriving=False):
        peer = other(*others[i])
        row = peer if arriving else me
        return send(gsum.at[row], gsum.at[row], g_s.at[i], g_r.at[i], {"dp": peer})

    @scoped
    def stage_g(_, __):
        for g in range(2):
            gsum[me, g : g + 1, :] = jnp.sum(gacc[g], axis=0, keepdims=True)
        for i in range(len(others)):
            gain_copy(i).start()

    @scoped
    def stage_h(_, __):
        for i, (dz, dy) in enumerate(others):
            j = others.index((dz, -dy % YN))
            peer = other(dz, dy)
            send(gsum.at[peer], gsum.at[peer], g_s.at[j], g_r.at[j], {"dp": peer}).wait_recv()
        gg[...] = jnp.sum(gsum[...], axis=0) * scale
        put(gg, gg_out)

    pl.semaphore_wait(barrier, len(others) + 2)
    stages = {
        "S": stage_s, "R": stage_r, "Q": stage_q, "C": stage_c, "P": stage_p, "Y": stage_y,
        "E": stage_e, "W": stage_w, "T": stage_t, "G": stage_g, "H": stage_h,
    }
    for step in ORDER:
        stages[step[0]](int(step[1]), int(step[2]))
    for st in range(4):
        gather_drain(st, ticks - 1)
        sum_drain(st, ticks - 1)
        for t in range(ticks - 1):
            shift(st, t).wait_send()
    for i in range(len(init_items)):
        gather_drain(4 + i, 0)
    for i in range(len(others)):
        gain_copy(i).wait_send()
    for copy in results:
        copy.wait()


def finish(act, cot, stash, gv, go, gg, *refs):
    n = 6
    outs, held, sems = refs[:n], refs[n : 2 * n], refs[2 * n]
    pieces = [
        (src.at[i], dst.at[0, i], mid.at[i])
        for src, dst, mid in zip((gv, go, stash, act, cot), (outs[3], outs[4], outs[2], outs[0], outs[1]), held)
        for i in range(src.shape[0])
    ]
    pieces.append((gg, outs[5].at[0], held[5]))
    for i, (src, _, mid) in enumerate(pieces):
        pltpu.make_async_copy(src, mid, sems.at[0, i]).start()
    for i, (src, dst, mid) in enumerate(pieces):
        pltpu.make_async_copy(src, mid, sems.at[0, i]).wait()
        pltpu.make_async_copy(mid, dst, sems.at[1, i]).start()
    for i, (_, dst, mid) in enumerate(pieces):
        pltpu.make_async_copy(mid, dst, sems.at[1, i]).wait()


def body(n_section, *args):
    w_value, w_out, norm_gain, saved, arriving, returning, fresh, targets, fill, read = args
    wv, wo, gain, saved, arr, ret = (
        a[0] for a in (w_value, w_out, norm_gain, saved, arriving, returning)
    )
    ticks, rows, depth = fresh.shape
    slots = saved.shape[0]
    feats = wv.shape[2]
    tokens = rows * YN * ZN
    vmem = pl.BlockSpec(memory_space=pltpu.VMEM)
    smem = pl.BlockSpec(memory_space=pltpu.SMEM)
    hbm = pl.BlockSpec(memory_space=pl.ANY)
    block = (rows, depth)
    n_rows = 4 + 2 * slots
    dma = pltpu.SemaphoreType.DMA
    held = [pltpu.VMEM(a.shape, a.dtype) for a in (wv, wo, saved, fresh, targets)]
    results = [((2, *block), BF16)] * 2 + [((slots, 2, *block), BF16), (wv.shape, BF16), (wo.shape, BF16), ((2, depth), F32)]
    outs = pl.pallas_call(
        functools.partial(window, n_section),
        out_shape=[jax.ShapeDtypeStruct(*r) for r in results],
        in_specs=[vmem] * 3 + [hbm] * 5 + [smem] * 2,
        out_specs=[hbm] * 6,
        scratch_shapes=[pltpu.VMEM(*r) for r in results]
        + held
        + [
            pltpu.VMEM((2 * ticks, 8, *block), BF16),
            pltpu.VMEM((2 * ticks, 8, *block), BF16),
            pltpu.VMEM((slots, 2, 8, *block), BF16),
            pltpu.VMEM((ticks, 2, *block), BF16),
            pltpu.VMEM((4, ZN, YN, *block), BF16),
            pltpu.VMEM((4, 2, ZN, rows, depth // 2), BF16),
            pltpu.VMEM((4, 2, ZN, *block), BF16),
            pltpu.VMEM((4, YN, *block), BF16),
            pltpu.VMEM((4, *block), F32),
            pltpu.VMEM((4, *block), BF16),
            pltpu.VMEM((4, *block), BF16),
            pltpu.VMEM((ticks, 2, *block), BF16),
            pltpu.VMEM((ticks, 2, *block), BF16),
            pltpu.VMEM((ticks - 1, 2, *block), BF16),
            pltpu.VMEM((ticks - 1, 2, *block), BF16),
            pltpu.VMEM((2, ticks * tokens, feats), BF16),
            pltpu.VMEM((2, *block), F32),
            pltpu.VMEM((8, 2, depth), F32),
            dma((len(held),)),
            dma((10,)),
            dma((n_rows, len(KEYS))),
            dma((n_rows, len(KEYS))),
            dma((4, 5)),
            dma((4, 5)),
            dma((ticks - 1, 4)),
            dma((ticks - 1, 4)),
            dma((7,)),
            dma((7,)),
        ],
        compiler_params=pltpu.CompilerParams(
            collective_id=0, has_side_effects=True, vmem_limit_bytes=VMEM_LIMIT
        ),
        name="window",
    )(gain, arr, ret, wv, wo, saved, fresh, targets, fill.swapaxes(1, 2), read.swapaxes(1, 2))
    return pl.pallas_call(
        finish,
        out_shape=[jax.ShapeDtypeStruct((1, *shape), dtype) for shape, dtype in results],
        in_specs=[hbm] * 6,
        out_specs=[hbm] * 6,
        scratch_shapes=[pltpu.VMEM(*results[i]) for i in (3, 4, 2, 0, 1, 5)] + [dma((2, 12))],
        compiler_params=pltpu.CompilerParams(vmem_limit_bytes=VMEM_LIMIT),
        name="finish",
    )(*outs)


def solution(mesh):
    in_specs = (
        P("section", None, None, "dp"),
        P("section", None, "dp", None),
        P("section", None, None),
        P("section", None, None, "dp", None),
        P("section", None, "dp", None),
        P("section", None, "dp", None),
        P(None, "dp", None),
        P(None, "dp", None),
        P("section", None, None),
        P("section", None, None),
    )
    out_specs = (
        P("section", None, "dp", None),
        P("section", None, "dp", None),
        P("section", None, None, "dp", None),
        P("section", None, None, "dp"),
        P("section", None, "dp", None),
        P("section", None, None),
    )
    return jax.shard_map(
        functools.partial(body, mesh.shape["section"]),
        mesh=mesh,
        in_specs=in_specs,
        out_specs=out_specs,
        check_vma=False,
    )
```

```python
import functools

import jax
import jax.numpy as jnp
from jax import lax
from jax.experimental import pallas as pl
from jax.experimental.pallas import tpu as pltpu
from jax.sharding import PartitionSpec as P

epsilon = 1e-06
MESH = pl.DeviceIdType.MESH
F32, BF16 = jnp.float32, jnp.bfloat16

F0, F1, B0, B1 = range(4)
YN, ZN = 4, 2

PIECES = {
    "y1": ((0, 0, None), 1),
    "y3": ((0, 0, None), -1),
    "z0": ((0, 0, None), "z"),
    "z1": ((0, -1, None), "z"),
    "z3": ((0, 1, None), "z"),
    "z2": ((0, 2, None), "z"),
    "w1": ((1, 0, None), 1),
    "w3": ((1, 0, None), -1),
    "h1": ((0, -1, 0), 1),
    "h3": ((0, 1, 1), -1),
    "v1": ((1, -1, 0), 1),
    "v3": ((1, 1, 1), -1),
}
KEYS = tuple(PIECES)
SUM_SENDS = {
    "Y": ("h1", "h3", "p1", "p3", "r1", "r3", "q2"),
    "Z": ("q2", "q1", "q3", "q0", "h1", "h3", "p1", "p3"),
}
SUM_KEYS = ("h1", "h3", "p1", "p3", "r1", "r3", "q2", "q1", "q3", "q0")
GATHERS = {
    "Y": {
        "S": ((), ("y1", "y3", "z0")),
        "R": (("y1", "y3"), ("h1", "h3", "z1", "z3")),
        "Q": (("h1", "h3"), ("z2",)),
        "C": (("z0", "z1", "z3", "z2"), ()),
    },
    "Z": {
        "S": ((), ("z0", "y1", "y3")),
        "R": (("z0", "y1", "y3"), ("w1", "w3", "h1", "h3")),
        "Q": (("w1", "w3"), ("v1", "v3")),
        "C": (("h1", "h3", "v1", "v3"), ()),
    },
}
STREAM_GATHERS = ("YZYZ", "YYZZ", "ZZYZ", "ZZZY")
STREAM_SUMS = ("YZYZ", "ZYYY", "YYZY", "YZYZ")
INIT_GATHERS = "YZZYZY"
ORDER = (
    "S00", "S30", "S20", "R00", "S10", "R30", "Q00", "R10", "R20", "Q30", "Q10", "S40",
    "C00", "Q20", "C30", "C10", "P00", "C20", "P10", "Y00", "P30", "Y10", "S80", "Y30",
    "E00", "P20", "E10", "E30", "S60", "Y20", "S01", "S11", "E20", "S31", "R01", "R11",
    "Q01", "S21", "R31", "Q11", "C01", "R21", "Q31", "C11", "Q21", "P01", "S50", "C31",
    "P11", "P31", "Y01", "Y11", "C21", "S70", "E01", "Y31", "E11", "P21", "R40", "R50",
    "E31", "Y21", "S02", "S12", "E21", "S32", "R02", "Q50", "R12", "Q40", "Q02", "S22",
    "R32", "R22", "Q12", "Q32", "C02", "Q22", "R70", "C12", "C32", "P02", "C22", "P32",
    "P22", "Y02", "P12", "Y32", "Y22", "E02", "R60", "Y12", "R80", "E32", "E22", "S90",
    "E12", "S03", "S33", "S23", "S13", "R33", "R23", "R03", "Q33", "Q23", "R90", "R13",
    "C33", "Q60", "Q03", "Q13", "Q80", "C23", "P33", "C03", "C13", "P23", "Y33", "W00",
    "P03", "Y23", "T00", "P13", "Q70", "E33", "Q90", "E23", "G00", "Y03", "Y13", "W10",
    "E03", "H00", "E13",
)
VMEM_LIMIT = 67043328


def scoped(stage):
    def run(*ids):
        with jax.named_scope("_".join([stage.__name__] + [str(i) for i in ids])):
            return stage(*ids)

    return run


def dot_nn(a, b):
    return jnp.dot(a, b, preferred_element_type=F32)


def dot_nt(a, b):
    return lax.dot_general(a, b, (((1,), (1,)), ((), ())), preferred_element_type=F32)


def dot_tn(a, b):
    return lax.dot_general(a, b, (((0,), (0,)), ((), ())), preferred_element_type=F32)


def window(
    n_section,
    gain_in, arr_in, ret_in, wv_in, wo_in, saved_in, fresh_in, tgt_in, fill, read,
    act_out, cot_out, stash_out, gv_out, go_out, gg_out,
    act, cot, stash, gv, go, gg,
    gain, arr, ret, wv, wo, saved, fresh, tgt,
    nrm, cotf, nsv, xin, part, rsh, rsy, zq, zs, zr, ysnd, dsnd, shf, shb, dgs, gacc, gsum,
    in_s, out_s, ag_s, ag_r, rs_s, rs_r, sh_s, sh_r, g_s, g_r,
):
    ticks = fresh.shape[0]
    slots = saved.shape[0]
    depth = gain.shape[1]
    half = depth // 2
    rows = arr.shape[1]
    tokens = rows * YN * ZN
    scale = (tokens * ticks) ** (-0.5)
    me = lax.axis_index("dp")
    sec = lax.axis_index("section")
    z, y = me // YN, me % YN
    zp = 1 - z
    first = sec == 0
    last = sec == n_section - 1
    nxt = lax.rem(sec + 1, n_section)
    prv = lax.rem(sec + n_section - 1, n_section)

    def y_at(k):
        return lax.rem(y + k + YN, YN)

    def to(where):
        if where == "z":
            return {"dp": zp * YN + y}
        return {"dp": z * YN + y_at(where)}

    others = [(dz, dy) for dz in range(ZN) for dy in range(YN) if dz or dy]

    def other(dz, dy):
        return (zp if dz else z) * YN + y_at(dy)

    barrier = pltpu.get_barrier_semaphore()
    for target in [{"dp": other(*o)} for o in others] + [{"section": nxt}, {"section": prv}]:
        pl.semaphore_signal(barrier, inc=1, device_id=target, device_id_type=MESH)

    loads = {
        "arr": (arr_in, arr),
        "gain": (gain_in, gain),
        "ret": (ret_in, ret),
        "wv": (wv_in, wv),
        "wo": (wo_in, wo),
        "saved": (saved_in, saved),
        "fresh": (fresh_in, fresh),
        "tgt": (tgt_in, tgt),
    }
    loads = {
        name: pltpu.make_async_copy(src, dst, in_s.at[i]) for i, (name, (src, dst)) in enumerate(loads.items())
    }
    for copy in loads.values():
        copy.start()
    loaded = set()

    def need(*names):
        for name in names:
            if name not in loaded:
                loads[name].wait()
                loaded.add(name)

    results = []

    def put(src, dst):
        copy = pltpu.make_async_copy(src, dst, out_s.at[len(results)])
        results.append(copy)
        copy.start()

    def send(src, dst, s, r, target):
        return pltpu.make_async_remote_copy(
            src_ref=src, dst_ref=dst, send_sem=s, recv_sem=r, device_id=target, device_id_type=MESH
        )

    def columns(h):
        return pl.ds(0, depth) if h is None else pl.ds(h * half, half)

    init_items = [(sl, g) for g in range(2) for sl in range(slots)]

    def mode_of(row, t):
        return STREAM_GATHERS[row][t] if row < 4 else INIT_GATHERS[row - 4]

    def over_y(st, t):
        return STREAM_SUMS[st][t] == "Y"

    def buf_of(row, t):
        if row >= 4:
            return nsv.at[init_items[row - 4]]
        return (nrm if row < B0 else cotf).at[2 * t + row % 2]

    def gather_copy(row, t, key, arriving=False):
        (dz, dy, h), where = PIECES[key]
        if arriving:
            dz, dy = (1 - dz, dy) if where == "z" else (dz, dy - where)
        block = buf_of(row, t).at[other(dz, dy), :, columns(h)]
        i = KEYS.index(key)
        return send(block, block, ag_s.at[row, i], ag_r.at[row, i], to(where))

    def gather(stage, row, t):
        waits, sends = GATHERS[mode_of(row, t)][stage]
        for key in waits:
            gather_copy(row, t, key, arriving=True).wait_recv()
        for key in sends:
            gather_copy(row, t, key).start()

    def gather_drain(row, t):
        for _, sends in GATHERS[mode_of(row, t)].values():
            for key in sends:
                gather_copy(row, t, key).wait_send()

    def sum_copy(st, t, key):
        i = SUM_KEYS.index(key)
        sems = (rs_s.at[st, i], rs_r.at[st, i])
        if key[0] == "q":
            if over_y(st, t):
                return send(zs.at[st], zr.at[st], *sems, to("z"))
            k = y_at(int(key[1]))
            return send(part.at[st, zp, k], zq.at[st, k], *sems, to("z"))
        way = 1 if key[1] == "1" else -1
        side = 0 if way == 1 else 1
        if key[0] == "h":
            n = ZN if over_y(st, t) else 1
            src = part.at[st, pl.ds(0 if over_y(st, t) else z, n), y_at(2), :, columns(side)]
            return send(src, rsh.at[st, side, pl.ds(0, n)], *sems, to(way))
        zz = zp if over_y(st, t) and key[0] == "p" else z
        at = zz if over_y(st, t) else 0
        return send(part.at[st, zz, y_at(way)], rsy.at[st, side, at], *sems, to(way))

    def sum_wait(st, t, *keys):
        for key in keys:
            sum_copy(st, t, key).wait_recv()

    def sum_start(st, t, *keys):
        for key in keys:
            sum_copy(st, t, key).start()

    def sum_drain(st, t):
        for key in SUM_SENDS[STREAM_SUMS[st][t]]:
            sum_copy(st, t, key).wait_send()

    def add_halves(st, zz, slot):
        for side, way in ((0, 1), (1, -1)):
            at = (st, zz, y_at(way), slice(None), columns(side))
            part[at] = (part[at].astype(F32) + rsh[st, side, slot].astype(F32)).astype(BF16)

    def shift(st, t):
        g = st % 2
        if st < B0:
            return send(ysnd.at[t, g], shf.at[t, g], sh_s.at[t, st], sh_r.at[t, st], {"section": nxt})
        return send(dsnd.at[t, g], shb.at[t, g], sh_s.at[t, st], sh_r.at[t, st], {"section": prv})

    def normed_of(x, g):
        inv = lax.rsqrt(jnp.mean(x * x, axis=-1, keepdims=True) + epsilon)
        scaled = x * inv
        return scaled, inv, (scaled * gain[g : g + 1, :]).astype(BF16)

    def whole(ref, i):
        return ref[i].astype(F32).reshape(tokens, depth).astype(BF16)

    @scoped
    def stage_s(st, t):
        if st >= 4:
            need("saved", "gain")
            sl, g = init_items[st - 4]
            buf_of(st, t)[me] = normed_of(saved[sl, g].astype(F32), g)[2]
            gather("S", st, t)
            return
        g = st % 2
        if t > 0:
            shift(st, t - 1).wait_recv()
        if st < B0:
            need("gain")
            if t == 0:
                need("arr")
                x = arr[g].astype(F32)
            else:
                need("fresh")
                edge = fresh[t] if g == 0 else shf[t - 1, 0]
                x = jnp.where(first, edge.astype(F32), shf[t - 1, g].astype(F32))
            xin[t, g] = x.astype(BF16)
            own = normed_of(x, g)[2]
        elif t == 0:
            need("ret")
            own = ret[g]
        else:
            if g == 0:
                edge = shb[t - 1, 1].astype(F32)
            else:
                need("tgt")
                edge = ysnd[t - 1, 1].astype(F32) - tgt[t - 1].astype(F32)
            own = jnp.where(last, edge, shb[t - 1, g].astype(F32)).astype(BF16)
        if t > 0:
            gather_drain(st, t - 1)
        buf_of(st, t)[me] = own
        gather("S", st, t)

    @scoped
    def stage_r(row, t):
        gather("R", row, t)

    @scoped
    def stage_q(row, t):
        gather("Q", row, t)

    @scoped
    def stage_c(st, t):
        g = st % 2
        gather("C", st, t)
        need("wv", "wo")
        if st < B0:
            values = dot_nn(whole(nrm, 2 * t + g), wv[g]).astype(BF16)
            terms = dot_nn(values, wo[g])
        else:
            down = dot_nt(whole(cotf, 2 * t + g), wo[g]).astype(BF16)
            dgs[g, t * tokens : (t + 1) * tokens, :] = down
            terms = dot_nt(down, wv[g])
        if t > 0:
            sum_drain(st, t - 1)
        part[st] = terms.reshape(ZN, YN, rows, depth).astype(BF16)
        if over_y(st, t):
            sum_start(st, t, "h1", "h3")
        else:
            sum_start(st, t, "q2", "q1", "q3", "q0")

    @scoped
    def stage_p(st, t):
        if over_y(st, t):
            sum_wait(st, t, "h1", "h3")
            add_halves(st, zp, zp)
            sum_start(st, t, "p1", "p3")
            add_halves(st, z, z)
            sum_start(st, t, "r1", "r3")
        else:
            sum_wait(st, t, "q2")
            add_block(st, 2)
            sum_start(st, t, "h1", "h3")

    @scoped
    def stage_y(st, t):
        if over_y(st, t):
            sum_wait(st, t, "p1", "p3")
            zs[st] = total_at(st, zp, zp).astype(BF16)
            sum_start(st, t, "q2")
        else:
            sum_wait(st, t, "q1", "q3")
            add_block(st, 1)
            add_block(st, 3)
            sum_wait(st, t, "h1", "h3")
            add_halves(st, z, 0)
            sum_start(st, t, "p1", "p3")

    def add_block(st, k):
        at = (st, z, y_at(k))
        part[at] = (part[at].astype(F32) + zq[st, y_at(k)].astype(F32)).astype(BF16)

    def total_at(st, zz, slot):
        acc = part[st, zz, y].astype(F32) + rsy[st, 0, slot].astype(F32)
        return acc + rsy[st, 1, slot].astype(F32)

    def pick(candidates, which):
        chosen = candidates[0][1]
        for index, value in candidates[1:]:
            chosen = jnp.where(index == which, value, chosen)
        return chosen

    def source_rows(t, g):
        options = [(sl, saved[sl, g].astype(F32)) for sl in range(slots)]
        options += [(fill[0, g, u], xin[u, g].astype(F32)) for u in range(t + 1)]
        return pick(options, read[0, g, t])

    @scoped
    def stage_e(st, t):
        g = st % 2
        if over_y(st, t):
            sum_wait(st, t, "r1", "r3", "q2")
            total = total_at(st, z, z) + zr[st].astype(F32)
        else:
            sum_wait(st, t, "q0", "p1", "p3")
            total = total_at(st, z, 0) + zq[st, y].astype(F32)
        if st < B0:
            out = (xin[t, g].astype(F32) + total).astype(BF16)
            ysnd[t, g] = out
        else:
            need("saved")
            scaled, inv, _ = normed_of(source_rows(t, g), g)
            weighted = total * gain[g : g + 1, :]
            inner = jnp.mean(weighted * scaled, axis=-1, keepdims=True)
            upstream = cotf[2 * t + g, me].astype(F32)
            out = (upstream + inv * (weighted - scaled * inner)).astype(BF16)
            dsnd[t, g] = out
            term = total * scaled
            gacc[g] = term if t == 0 else gacc[g] + term
        if t > 0:
            shift(st, t - 1).wait_send()
        if t == ticks - 1:
            gather_drain(st, t)
        if t < ticks - 1:
            shift(st, t).start()
        elif st < B0:
            act[g] = out
            put(act.at[g], act_out.at[g])
        else:
            cot[g] = out
            put(cot.at[g], cot_out.at[g])

    @scoped
    def stage_w(g, _):
        for i in range(slots):
            gather("C", 4 + g * slots + i, 0)
            gather_drain(4 + g * slots + i, 0)
        picked = []
        for t in range(ticks):
            options = [(sl, nsv[sl, g].astype(F32)) for sl in range(slots)]
            options += [(fill[0, g, u], nrm[2 * u + g].astype(F32)) for u in range(t + 1)]
            picked.append(pick(options, read[0, g, t]).reshape(tokens, depth).astype(BF16))
        normed = jnp.concatenate(picked, axis=0)
        values = dot_nn(normed, wv[g]).astype(BF16)
        gv[g] = (dot_tn(normed, dgs[g]) * scale).astype(BF16)
        put(gv.at[g], gv_out.at[g])
        upstream = jnp.concatenate([whole(cotf, 2 * t + g) for t in range(ticks)], axis=0)
        go[g] = (dot_tn(values, upstream) * scale).astype(BF16)
        put(go.at[g], go_out.at[g])

    @scoped
    def stage_t(_, __):
        for sl in range(slots):
            for g in range(2):
                rows_now = saved[sl, g].astype(F32)
                for t in range(ticks):
                    rows_now = jnp.where(fill[0, g, t] == sl, xin[t, g].astype(F32), rows_now)
                stash[sl, g] = rows_now.astype(BF16)
        put(stash, stash_out)

    def gain_copy(i, arriving=False):
        peer = other(*others[i])
        row = peer if arriving else me
        return send(gsum.at[row], gsum.at[row], g_s.at[i], g_r.at[i], {"dp": peer})

    @scoped
    def stage_g(_, __):
        for g in range(2):
            gsum[me, g : g + 1, :] = jnp.sum(gacc[g], axis=0, keepdims=True)
        for i in range(len(others)):
            gain_copy(i).start()

    @scoped
    def stage_h(_, __):
        for i, (dz, dy) in enumerate(others):
            j = others.index((dz, -dy % YN))
            peer = other(dz, dy)
            send(gsum.at[peer], gsum.at[peer], g_s.at[j], g_r.at[j], {"dp": peer}).wait_recv()
        gg[...] = jnp.sum(gsum[...], axis=0) * scale
        put(gg, gg_out)

    need("arr", "gain", "ret")
    pl.semaphore_wait(barrier, len(others) + 2)
    stages = {
        "S": stage_s, "R": stage_r, "Q": stage_q, "C": stage_c, "P": stage_p, "Y": stage_y,
        "E": stage_e, "W": stage_w, "T": stage_t, "G": stage_g, "H": stage_h,
    }
    for step in ORDER:
        stages[step[0]](int(step[1]), int(step[2]))
    for st in range(4):
        sum_drain(st, ticks - 1)
    for i in range(len(others)):
        gain_copy(i).wait_send()
    for copy in results:
        copy.wait()


def finish(act, cot, stash, gv, go, gg, *refs):
    n = 6
    outs, held, sems = refs[:n], refs[n : 2 * n], refs[2 * n]
    pieces = [
        (src.at[i], dst.at[0, i], mid.at[i])
        for src, dst, mid in zip((gv, go, stash, act, cot), (outs[3], outs[4], outs[2], outs[0], outs[1]), held)
        for i in range(src.shape[0])
    ]
    pieces.append((gg, outs[5].at[0], held[5]))
    for i, (src, _, mid) in enumerate(pieces):
        pltpu.make_async_copy(src, mid, sems.at[0, i]).start()
    for i, (src, dst, mid) in enumerate(pieces):
        pltpu.make_async_copy(src, mid, sems.at[0, i]).wait()
        pltpu.make_async_copy(mid, dst, sems.at[1, i]).start()
    for i, (_, dst, mid) in enumerate(pieces):
        pltpu.make_async_copy(mid, dst, sems.at[1, i]).wait()


def body(n_section, *args):
    w_value, w_out, norm_gain, saved, arriving, returning, fresh, targets, fill, read = args
    wv, wo, gain, saved, arr, ret = (
        a[0] for a in (w_value, w_out, norm_gain, saved, arriving, returning)
    )
    ticks, rows, depth = fresh.shape
    slots = saved.shape[0]
    feats = wv.shape[2]
    tokens = rows * YN * ZN
    smem = pl.BlockSpec(memory_space=pltpu.SMEM)
    hbm = pl.BlockSpec(memory_space=pl.ANY)
    block = (rows, depth)
    n_rows = 4 + 2 * slots
    dma = pltpu.SemaphoreType.DMA
    held = [pltpu.VMEM(a.shape, a.dtype) for a in (gain, arr, ret, wv, wo, saved, fresh, targets)]
    results = [((2, *block), BF16)] * 2 + [((slots, 2, *block), BF16), (wv.shape, BF16), (wo.shape, BF16), ((2, depth), F32)]
    outs = pl.pallas_call(
        functools.partial(window, n_section),
        out_shape=[jax.ShapeDtypeStruct(*r) for r in results],
        in_specs=[hbm] * 8 + [smem] * 2,
        out_specs=[hbm] * 6,
        scratch_shapes=[pltpu.VMEM(*r) for r in results]
        + held
        + [
            pltpu.VMEM((2 * ticks, 8, *block), BF16),
            pltpu.VMEM((2 * ticks, 8, *block), BF16),
            pltpu.VMEM((slots, 2, 8, *block), BF16),
            pltpu.VMEM((ticks, 2, *block), BF16),
            pltpu.VMEM((4, ZN, YN, *block), BF16),
            pltpu.VMEM((4, 2, ZN, rows, depth // 2), BF16),
            pltpu.VMEM((4, 2, ZN, *block), BF16),
            pltpu.VMEM((4, YN, *block), BF16),
            pltpu.VMEM((4, *block), BF16),
            pltpu.VMEM((4, *block), BF16),
            pltpu.VMEM((ticks, 2, *block), BF16),
            pltpu.VMEM((ticks, 2, *block), BF16),
            pltpu.VMEM((ticks - 1, 2, *block), BF16),
            pltpu.VMEM((ticks - 1, 2, *block), BF16),
            pltpu.VMEM((2, ticks * tokens, feats), BF16),
            pltpu.VMEM((2, *block), F32),
            pltpu.VMEM((8, 2, depth), F32),
            dma((len(held),)),
            dma((10,)),
            dma((n_rows, len(KEYS))),
            dma((n_rows, len(KEYS))),
            dma((4, len(SUM_KEYS))),
            dma((4, len(SUM_KEYS))),
            dma((ticks - 1, 4)),
            dma((ticks - 1, 4)),
            dma((7,)),
            dma((7,)),
        ],
        compiler_params=pltpu.CompilerParams(
            collective_id=0, has_side_effects=True, vmem_limit_bytes=VMEM_LIMIT
        ),
        name="window",
    )(gain, arr, ret, wv, wo, saved, fresh, targets, fill.swapaxes(1, 2), read.swapaxes(1, 2))
    return pl.pallas_call(
        finish,
        out_shape=[jax.ShapeDtypeStruct((1, *shape), dtype) for shape, dtype in results],
        in_specs=[hbm] * 6,
        out_specs=[hbm] * 6,
        scratch_shapes=[pltpu.VMEM(*results[i]) for i in (3, 4, 2, 0, 1, 5)] + [dma((2, 12))],
        compiler_params=pltpu.CompilerParams(vmem_limit_bytes=VMEM_LIMIT),
        name="finish",
    )(*outs)


def solution(mesh):
    in_specs = (
        P("section", None, None, "dp"),
        P("section", None, "dp", None),
        P("section", None, None),
        P("section", None, None, "dp", None),
        P("section", None, "dp", None),
        P("section", None, "dp", None),
        P(None, "dp", None),
        P(None, "dp", None),
        P("section", None, None),
        P("section", None, None),
    )
    out_specs = (
        P("section", None, "dp", None),
        P("section", None, "dp", None),
        P("section", None, None, "dp", None),
        P("section", None, None, "dp"),
        P("section", None, "dp", None),
        P("section", None, None),
    )
    return jax.shard_map(
        functools.partial(body, mesh.shape["section"]),
        mesh=mesh,
        in_specs=in_specs,
        out_specs=out_specs,
        check_vma=False,
    )
```

```python
import functools

import jax
import jax.numpy as jnp
from jax import lax
from jax.experimental import pallas as pl
from jax.experimental.pallas import tpu as pltpu
from jax.sharding import PartitionSpec as P

epsilon = 1e-06
MESH = pl.DeviceIdType.MESH
F32, BF16 = jnp.float32, jnp.bfloat16

F0, F1, B0, B1 = range(4)
YN, ZN = 4, 2

PIECES = {
    "y1": ((0, 0, None), 1),
    "y3": ((0, 0, None), -1),
    "z0": ((0, 0, None), "z"),
    "z1": ((0, -1, None), "z"),
    "z3": ((0, 1, None), "z"),
    "z2": ((0, 2, None), "z"),
    "w1": ((1, 0, None), 1),
    "w3": ((1, 0, None), -1),
    "h1": ((0, -1, 0), 1),
    "h3": ((0, 1, 1), -1),
    "v1": ((1, -1, 0), 1),
    "v3": ((1, 1, 1), -1),
}
KEYS = tuple(PIECES)
SUM_SENDS = {
    "Y": ("h1", "h3", "p1", "p3", "r1", "r3", "q2"),
    "Z": ("q2", "q1", "q3", "q0", "h1", "h3", "p1", "p3"),
}
SUM_KEYS = ("h1", "h3", "p1", "p3", "r1", "r3", "q2", "q1", "q3", "q0")
GATHERS = {
    "Y": {
        "S": ((), ("y1", "y3", "z0")),
        "R": (("y1", "y3"), ("h1", "h3", "z1", "z3")),
        "Q": (("h1", "h3"), ("z2",)),
        "C": (("z0", "z1", "z3", "z2"), ()),
    },
    "Z": {
        "S": ((), ("z0", "y1", "y3")),
        "R": (("z0", "y1", "y3"), ("w1", "w3", "h1", "h3")),
        "Q": (("w1", "w3"), ("v1", "v3")),
        "C": (("h1", "h3", "v1", "v3"), ()),
    },
}
STREAM_GATHERS = ("YZYZ", "YYZZ", "ZZYZ", "ZZZY")
STREAM_SUMS = ("YZYZ", "ZYYY", "YYZY", "YZYZ")
INIT_GATHERS = "YZZYZY"
ORDER = (
    "S00", "S30", "S20", "R00", "S10", "R30", "Q00", "R10", "R20", "Q30", "Q10", "S40",
    "C00", "Q20", "C30", "C10", "P00", "C20", "P10", "Y00", "P30", "Y10", "S80", "Y30",
    "E00", "P20", "E10", "E30", "S60", "Y20", "S01", "S11", "E20", "S31", "R01", "R11",
    "Q01", "S21", "R31", "Q11", "C01", "R21", "Q31", "C11", "Q21", "P01", "S50", "C31",
    "P11", "P31", "Y01", "Y11", "C21", "S70", "E01", "Y31", "E11", "P21", "R40", "R50",
    "E31", "Y21", "S02", "S12", "E21", "S32", "R02", "Q50", "R12", "Q40", "Q02", "S22",
    "R32", "R22", "Q12", "Q32", "C02", "Q22", "R70", "C12", "C32", "P02", "C22", "P32",
    "P22", "Y02", "P12", "Y32", "Y22", "E02", "R60", "Y12", "R80", "E32", "E22", "S90",
    "E12", "S03", "S33", "S23", "S13", "R33", "R23", "R03", "Q33", "Q23", "R90", "R13",
    "C33", "Q60", "Q03", "Q13", "Q80", "C23", "P33", "C03", "C13", "P23", "Y33", "W00",
    "P03", "Y23", "T00", "P13", "Q70", "E33", "Q90", "E23", "G00", "Y03", "Y13", "W10",
    "E03", "H00", "E13",
)
VMEM_LIMIT = 67043328


def scoped(stage):
    def run(*ids):
        with jax.named_scope("_".join([stage.__name__] + [str(i) for i in ids])):
            return stage(*ids)

    return run


def dot_nn(a, b):
    return jnp.dot(a, b, preferred_element_type=F32)


def dot_nt(a, b):
    return lax.dot_general(a, b, (((1,), (1,)), ((), ())), preferred_element_type=F32)


def dot_tn(a, b):
    return lax.dot_general(a, b, (((0,), (0,)), ((), ())), preferred_element_type=F32)


def window(
    n_section,
    gain_in, arr_in, ret_in, wv_in, wo_in, saved_in, fresh_in, tgt_in, fill, read,
    act_out, cot_out, stash_out, gv_out, go_out, gg_out,
    act, cot, stash, gv, go, gg,
    gain, arr, ret, wv, wo, saved, fresh, tgt,
    nrm, cotf, nsv, xin, part, rsh, rsy, zq, zs, zr, ysnd, dsnd, shf, shb, dgs, gacc, gsum,
    in_s, out_s, ag_s, ag_r, rs_s, rs_r, sh_s, sh_r, g_s, g_r,
):
    ticks = fresh.shape[0]
    slots = saved.shape[0]
    depth = gain.shape[1]
    half = depth // 2
    rows = arr.shape[1]
    tokens = rows * YN * ZN
    scale = (tokens * ticks) ** (-0.5)
    me = lax.axis_index("dp")
    sec = lax.axis_index("section")
    z, y = me // YN, me % YN
    zp = 1 - z
    first = sec == 0
    last = sec == n_section - 1
    nxt = lax.rem(sec + 1, n_section)
    prv = lax.rem(sec + n_section - 1, n_section)

    def y_at(k):
        return lax.rem(y + k + YN, YN)

    def to(where):
        if where == "z":
            return {"dp": zp * YN + y}
        return {"dp": z * YN + y_at(where)}

    others = [(dz, dy) for dz in range(ZN) for dy in range(YN) if dz or dy]

    def other(dz, dy):
        return (zp if dz else z) * YN + y_at(dy)

    barrier = pltpu.get_barrier_semaphore()
    for target in [{"dp": other(*o)} for o in others] + [{"section": nxt}, {"section": prv}]:
        pl.semaphore_signal(barrier, inc=1, device_id=target, device_id_type=MESH)

    loads = {
        "arr": (arr_in, arr),
        "gain": (gain_in, gain),
        "ret": (ret_in, ret),
        "wv": (wv_in, wv),
        "wo": (wo_in, wo),
        "saved": (saved_in, saved),
        "fresh": (fresh_in, fresh),
        "tgt": (tgt_in, tgt),
    }
    loads = {
        name: pltpu.make_async_copy(src, dst, in_s.at[i]) for i, (name, (src, dst)) in enumerate(loads.items())
    }
    for copy in loads.values():
        copy.start()
    loaded = set()

    def need(*names):
        for name in names:
            if name not in loaded:
                loads[name].wait()
                loaded.add(name)

    results = []

    def put(src, dst):
        copy = pltpu.make_async_copy(src, dst, out_s.at[len(results)])
        results.append(copy)
        copy.start()

    def send(src, dst, s, r, target):
        return pltpu.make_async_remote_copy(
            src_ref=src, dst_ref=dst, send_sem=s, recv_sem=r, device_id=target, device_id_type=MESH
        )

    def columns(h):
        return pl.ds(0, depth) if h is None else pl.ds(h * half, half)

    init_items = [(sl, g) for g in range(2) for sl in range(slots)]

    def mode_of(row, t):
        return STREAM_GATHERS[row][t] if row < 4 else INIT_GATHERS[row - 4]

    def over_y(st, t):
        return STREAM_SUMS[st][t] == "Y"

    def buf_of(row, t):
        if row >= 4:
            return nsv.at[init_items[row - 4]]
        return (nrm if row < B0 else cotf).at[2 * t + row % 2]

    def gather_copy(row, t, key, arriving=False):
        (dz, dy, h), where = PIECES[key]
        if arriving:
            dz, dy = (1 - dz, dy) if where == "z" else (dz, dy - where)
        block = buf_of(row, t).at[other(dz, dy), :, columns(h)]
        i = KEYS.index(key)
        return send(block, block, ag_s.at[row, i], ag_r.at[row, i], to(where))

    def gather(stage, row, t):
        waits, sends = GATHERS[mode_of(row, t)][stage]
        for key in waits:
            gather_copy(row, t, key, arriving=True).wait_recv()
        for key in sends:
            gather_copy(row, t, key).start()

    def gather_drain(row, t):
        for _, sends in GATHERS[mode_of(row, t)].values():
            for key in sends:
                gather_copy(row, t, key).wait_send()

    def sum_copy(st, t, key):
        i = SUM_KEYS.index(key)
        sems = (rs_s.at[st, i], rs_r.at[st, i])
        if key[0] == "q":
            if over_y(st, t):
                return send(zs.at[st], zr.at[st], *sems, to("z"))
            k = y_at(int(key[1]))
            return send(part.at[st, zp, k], zq.at[st, k], *sems, to("z"))
        way = 1 if key[1] == "1" else -1
        side = 0 if way == 1 else 1
        if key[0] == "h":
            n = ZN if over_y(st, t) else 1
            src = part.at[st, pl.ds(0 if over_y(st, t) else z, n), y_at(2), :, columns(side)]
            return send(src, rsh.at[st, side, pl.ds(0, n)], *sems, to(way))
        zz = zp if over_y(st, t) and key[0] == "p" else z
        at = zz if over_y(st, t) else 0
        return send(part.at[st, zz, y_at(way)], rsy.at[st, side, at], *sems, to(way))

    def sum_wait(st, t, *keys):
        for key in keys:
            sum_copy(st, t, key).wait_recv()

    def sum_start(st, t, *keys):
        for key in keys:
            sum_copy(st, t, key).start()

    def sum_drain(st, t):
        for key in SUM_SENDS[STREAM_SUMS[st][t]]:
            sum_copy(st, t, key).wait_send()

    def add_halves(st, zz, slot):
        for side, way in ((0, 1), (1, -1)):
            at = (st, zz, y_at(way), slice(None), columns(side))
            part[at] = (part[at].astype(F32) + rsh[st, side, slot].astype(F32)).astype(BF16)

    def shift(st, t):
        g = st % 2
        if st < B0:
            return send(ysnd.at[t, g], shf.at[t, g], sh_s.at[t, st], sh_r.at[t, st], {"section": nxt})
        return send(dsnd.at[t, g], shb.at[t, g], sh_s.at[t, st], sh_r.at[t, st], {"section": prv})

    def normed_of(x, g):
        inv = lax.rsqrt(jnp.mean(x * x, axis=-1, keepdims=True) + epsilon)
        scaled = x * inv
        return scaled, inv, (scaled * gain[g : g + 1, :]).astype(BF16)

    def whole(ref, i):
        return ref[i].astype(F32).reshape(tokens, depth).astype(BF16)

    @scoped
    def stage_s(st, t):
        if st >= 4:
            need("saved", "gain")
            sl, g = init_items[st - 4]
            buf_of(st, t)[me] = normed_of(saved[sl, g].astype(F32), g)[2]
            gather("S", st, t)
            return
        g = st % 2
        if t > 0:
            shift(st, t - 1).wait_recv()
        if st < B0:
            need("gain")
            if t == 0:
                need("arr")
                x = arr[g].astype(F32)
            else:
                need("fresh")
                edge = fresh[t] if g == 0 else shf[t - 1, 0]
                x = jnp.where(first, edge.astype(F32), shf[t - 1, g].astype(F32))
            xin[t, g] = x.astype(BF16)
            own = normed_of(x, g)[2]
        elif t == 0:
            need("ret")
            own = ret[g]
        else:
            if g == 0:
                edge = shb[t - 1, 1].astype(F32)
            else:
                need("tgt")
                edge = ysnd[t - 1, 1].astype(F32) - tgt[t - 1].astype(F32)
            own = jnp.where(last, edge, shb[t - 1, g].astype(F32)).astype(BF16)
        if t > 0:
            gather_drain(st, t - 1)
        buf_of(st, t)[me] = own
        gather("S", st, t)

    @scoped
    def stage_r(row, t):
        gather("R", row, t)

    @scoped
    def stage_q(row, t):
        gather("Q", row, t)

    @scoped
    def stage_c(st, t):
        g = st % 2
        gather("C", st, t)
        need("wv", "wo")
        if st < B0:
            values = dot_nn(whole(nrm, 2 * t + g), wv[g]).astype(BF16)
            terms = dot_nn(values, wo[g])
        else:
            down = dot_nt(whole(cotf, 2 * t + g), wo[g]).astype(BF16)
            dgs[g, t * tokens : (t + 1) * tokens, :] = down
            terms = dot_nt(down, wv[g])
        if t > 0:
            sum_drain(st, t - 1)
        part[st] = terms.reshape(ZN, YN, rows, depth).astype(BF16)
        if over_y(st, t):
            sum_start(st, t, "h1", "h3")
        else:
            sum_start(st, t, "q2", "q1", "q3", "q0")

    @scoped
    def stage_p(st, t):
        if over_y(st, t):
            sum_wait(st, t, "h1", "h3")
            add_halves(st, zp, zp)
            sum_start(st, t, "p1", "p3")
            add_halves(st, z, z)
            sum_start(st, t, "r1", "r3")
        else:
            sum_wait(st, t, "q2")
            add_block(st, 2)
            sum_start(st, t, "h1", "h3")

    @scoped
    def stage_y(st, t):
        if over_y(st, t):
            sum_wait(st, t, "p1", "p3")
            zs[st] = total_at(st, zp, zp).astype(BF16)
            sum_start(st, t, "q2")
        else:
            sum_wait(st, t, "q1", "q3")
            add_block(st, 1)
            add_block(st, 3)
            sum_wait(st, t, "h1", "h3")
            add_halves(st, z, 0)
            sum_start(st, t, "p1", "p3")

    def add_block(st, k):
        at = (st, z, y_at(k))
        part[at] = (part[at].astype(F32) + zq[st, y_at(k)].astype(F32)).astype(BF16)

    def total_at(st, zz, slot):
        acc = part[st, zz, y].astype(F32) + rsy[st, 0, slot].astype(F32)
        return acc + rsy[st, 1, slot].astype(F32)

    def pick(candidates, which):
        chosen = candidates[0][1]
        for index, value in candidates[1:]:
            chosen = jnp.where(index == which, value, chosen)
        return chosen

    def source_rows(t, g):
        options = [(sl, saved[sl, g].astype(F32)) for sl in range(slots)]
        options += [(fill[0, g, u], xin[u, g].astype(F32)) for u in range(t + 1)]
        return pick(options, read[0, g, t])

    @scoped
    def stage_e(st, t):
        g = st % 2
        if over_y(st, t):
            sum_wait(st, t, "r1", "r3", "q2")
            total = total_at(st, z, z) + zr[st].astype(F32)
        else:
            sum_wait(st, t, "q0", "p1", "p3")
            total = total_at(st, z, 0) + zq[st, y].astype(F32)
        if st < B0:
            out = (xin[t, g].astype(F32) + total).astype(BF16)
            ysnd[t, g] = out
        else:
            need("saved")
            scaled, inv, _ = normed_of(source_rows(t, g), g)
            weighted = total * gain[g : g + 1, :]
            inner = jnp.mean(weighted * scaled, axis=-1, keepdims=True)
            upstream = cotf[2 * t + g, me].astype(F32)
            out = (upstream + inv * (weighted - scaled * inner)).astype(BF16)
            dsnd[t, g] = out
            term = total * scaled
            gacc[g] = term if t == 0 else gacc[g] + term
        if t > 0:
            shift(st, t - 1).wait_send()
        if t == ticks - 1:
            gather_drain(st, t)
        if t < ticks - 1:
            shift(st, t).start()
        elif st < B0:
            act[g] = out
            put(act.at[g], act_out.at[g])
        else:
            cot[g] = out
            put(cot.at[g], cot_out.at[g])

    @scoped
    def stage_w(g, _):
        for i in range(slots):
            gather("C", 4 + g * slots + i, 0)
            gather_drain(4 + g * slots + i, 0)
        picked = []
        for t in range(ticks):
            options = [(sl, nsv[sl, g].astype(F32)) for sl in range(slots)]
            options += [(fill[0, g, u], nrm[2 * u + g].astype(F32)) for u in range(t + 1)]
            picked.append(pick(options, read[0, g, t]).reshape(tokens, depth).astype(BF16))
        normed = jnp.concatenate(picked, axis=0)
        values = dot_nn(normed, wv[g]).astype(BF16)
        gv[g] = (dot_tn(normed, dgs[g]) * scale).astype(BF16)
        put(gv.at[g], gv_out.at[g])
        upstream = jnp.concatenate([whole(cotf, 2 * t + g) for t in range(ticks)], axis=0)
        go[g] = (dot_tn(values, upstream) * scale).astype(BF16)
        put(go.at[g], go_out.at[g])

    @scoped
    def stage_t(_, __):
        for sl in range(slots):
            for g in range(2):
                rows_now = saved[sl, g].astype(F32)
                for t in range(ticks):
                    rows_now = jnp.where(fill[0, g, t] == sl, xin[t, g].astype(F32), rows_now)
                stash[sl, g] = rows_now.astype(BF16)
        put(stash, stash_out)

    def gain_copy(i, arriving=False):
        peer = other(*others[i])
        row = peer if arriving else me
        return send(gsum.at[row], gsum.at[row], g_s.at[i], g_r.at[i], {"dp": peer})

    @scoped
    def stage_g(_, __):
        sums = [jnp.sum(gacc[g], axis=0, keepdims=True) for g in range(2)]
        gsum[me] = jnp.concatenate(sums, axis=0).astype(BF16)
        for i in range(len(others)):
            gain_copy(i).start()

    @scoped
    def stage_h(_, __):
        for i, (dz, dy) in enumerate(others):
            j = others.index((dz, -dy % YN))
            peer = other(dz, dy)
            send(gsum.at[peer], gsum.at[peer], g_s.at[j], g_r.at[j], {"dp": peer}).wait_recv()
        gg[...] = jnp.sum(gsum[...].astype(F32), axis=0) * scale
        put(gg, gg_out)

    need("arr", "gain", "ret")
    pl.semaphore_wait(barrier, len(others) + 2)
    stages = {
        "S": stage_s, "R": stage_r, "Q": stage_q, "C": stage_c, "P": stage_p, "Y": stage_y,
        "E": stage_e, "W": stage_w, "T": stage_t, "G": stage_g, "H": stage_h,
    }
    for step in ORDER:
        stages[step[0]](int(step[1]), int(step[2]))
    for st in range(4):
        sum_drain(st, ticks - 1)
    for i in range(len(others)):
        gain_copy(i).wait_send()
    for copy in results:
        copy.wait()


def finish(act, cot, stash, gv, go, gg, *refs):
    n = 6
    outs, held, sems = refs[:n], refs[n : 2 * n], refs[2 * n]
    pieces = []
    for src, dst, mid, cuts in zip((gv, go, stash, act, cot), (outs[3], outs[4], outs[2], outs[0], outs[1]), held, (4, 4, 1, 1, 1)):
        for i in range(src.shape[0]):
            n_rows = src.shape[1] // cuts
            for c in range(cuts):
                part = pl.ds(c * n_rows, n_rows)
                pieces.append((src.at[i, part], dst.at[0, i, part], mid.at[i, part]))
    pieces.append((gg, outs[5].at[0], held[5]))
    for i, (src, _, mid) in enumerate(pieces):
        pltpu.make_async_copy(src, mid, sems.at[0, i]).start()
    for i, (src, dst, mid) in enumerate(pieces):
        pltpu.make_async_copy(src, mid, sems.at[0, i]).wait()
        pltpu.make_async_copy(mid, dst, sems.at[1, i]).start()
    for i, (_, dst, mid) in enumerate(pieces):
        pltpu.make_async_copy(mid, dst, sems.at[1, i]).wait()


def body(n_section, *args):
    w_value, w_out, norm_gain, saved, arriving, returning, fresh, targets, fill, read = args
    wv, wo, gain, saved, arr, ret = (
        a[0] for a in (w_value, w_out, norm_gain, saved, arriving, returning)
    )
    ticks, rows, depth = fresh.shape
    slots = saved.shape[0]
    feats = wv.shape[2]
    tokens = rows * YN * ZN
    smem = pl.BlockSpec(memory_space=pltpu.SMEM)
    hbm = pl.BlockSpec(memory_space=pl.ANY)
    block = (rows, depth)
    n_rows = 4 + 2 * slots
    dma = pltpu.SemaphoreType.DMA
    held = [pltpu.VMEM(a.shape, a.dtype) for a in (gain, arr, ret, wv, wo, saved, fresh, targets)]
    results = [((2, *block), BF16)] * 2 + [((slots, 2, *block), BF16), (wv.shape, BF16), (wo.shape, BF16), ((2, depth), F32)]
    outs = pl.pallas_call(
        functools.partial(window, n_section),
        out_shape=[jax.ShapeDtypeStruct(*r) for r in results],
        in_specs=[hbm] * 8 + [smem] * 2,
        out_specs=[hbm] * 6,
        scratch_shapes=[pltpu.VMEM(*r) for r in results]
        + held
        + [
            pltpu.VMEM((2 * ticks, 8, *block), BF16),
            pltpu.VMEM((2 * ticks, 8, *block), BF16),
            pltpu.VMEM((slots, 2, 8, *block), BF16),
            pltpu.VMEM((ticks, 2, *block), BF16),
            pltpu.VMEM((4, ZN, YN, *block), BF16),
            pltpu.VMEM((4, 2, ZN, rows, depth // 2), BF16),
            pltpu.VMEM((4, 2, ZN, *block), BF16),
            pltpu.VMEM((4, YN, *block), BF16),
            pltpu.VMEM((4, *block), BF16),
            pltpu.VMEM((4, *block), BF16),
            pltpu.VMEM((ticks, 2, *block), BF16),
            pltpu.VMEM((ticks, 2, *block), BF16),
            pltpu.VMEM((ticks - 1, 2, *block), BF16),
            pltpu.VMEM((ticks - 1, 2, *block), BF16),
            pltpu.VMEM((2, ticks * tokens, feats), BF16),
            pltpu.VMEM((2, *block), F32),
            pltpu.VMEM((8, 2, depth), BF16),
            dma((len(held),)),
            dma((10,)),
            dma((n_rows, len(KEYS))),
            dma((n_rows, len(KEYS))),
            dma((4, len(SUM_KEYS))),
            dma((4, len(SUM_KEYS))),
            dma((ticks - 1, 4)),
            dma((ticks - 1, 4)),
            dma((7,)),
            dma((7,)),
        ],
        compiler_params=pltpu.CompilerParams(
            collective_id=0, has_side_effects=True, vmem_limit_bytes=VMEM_LIMIT
        ),
        name="window",
    )(gain, arr, ret, wv, wo, saved, fresh, targets, fill.swapaxes(1, 2), read.swapaxes(1, 2))
    return pl.pallas_call(
        finish,
        out_shape=[jax.ShapeDtypeStruct((1, *shape), dtype) for shape, dtype in results],
        in_specs=[hbm] * 6,
        out_specs=[hbm] * 6,
        scratch_shapes=[pltpu.VMEM(*results[i]) for i in (3, 4, 2, 0, 1, 5)] + [dma((2, 24))],
        compiler_params=pltpu.CompilerParams(vmem_limit_bytes=VMEM_LIMIT),
        name="finish",
    )(*outs)


def solution(mesh):
    in_specs = (
        P("section", None, None, "dp"),
        P("section", None, "dp", None),
        P("section", None, None),
        P("section", None, None, "dp", None),
        P("section", None, "dp", None),
        P("section", None, "dp", None),
        P(None, "dp", None),
        P(None, "dp", None),
        P("section", None, None),
        P("section", None, None),
    )
    out_specs = (
        P("section", None, "dp", None),
        P("section", None, "dp", None),
        P("section", None, None, "dp", None),
        P("section", None, None, "dp"),
        P("section", None, "dp", None),
        P("section", None, None),
    )
    return jax.shard_map(
        functools.partial(body, mesh.shape["section"]),
        mesh=mesh,
        in_specs=in_specs,
        out_specs=out_specs,
        check_vma=False,
    )
```
